32 devices in a mesh: gx: 4 (over z), gy: 4 (over y, x), gz: 2 (over core).
Axes of the slice: x: 2, y: 2, z: 4, core: 2. Of those that a mesh axis runs over, the one named last changes fastest.
Arguments:
- signal: float32 [16, 131072], P(None, ('gx', 'gy', 'gz')), may hold values from -6 to 6
- order: int32 [131072], P(('gx', 'gy', 'gz')), may hold values from 0 to 4095, as said below
- near_tiles: bfloat16 [512, 3, 256, 256], P(('gx', 'gy', 'gz')), may hold values from -0.21875 to 0.21875
- near_list: int32 [512, 3], P(('gx', 'gy', 'gz')), may hold values from 0 to 511, as said below
- leaf_basis: bfloat16 [512, 64, 256], P(('gx', 'gy', 'gz')), may hold values from -0.375 to 0.375
- leaf_transfer: bfloat16 [512, 64, 64], P(('gx', 'gy', 'gz')), may hold values from -0.5 to 0.5
- leaf_coupling: bfloat16 [512, 64, 192], P(('gx', 'gy', 'gz')), may hold values from -0.4375 to 0.4375
- leaf_links: int32 [512, 3], P(('gx', 'gy', 'gz')), may hold values from 0 to 511, as said below
- device_transfer: bfloat16 [32, 64, 64], P(('gx', 'gy', 'gz')), may hold values from -0.5 to 0.5
- device_coupling: bfloat16 [32, 64, 192], P(('gx', 'gy', 'gz')), may hold values from -0.15625 to 0.15625
- device_links: int32 [32, 3], P(('gx', 'gy', 'gz')), may hold values from 0 to 31, as said below
- block_transfer: bfloat16 [16, 64, 64], P(('gx', 'gy')), may hold values from -0.5 to 0.5
- block_coupling: bfloat16 [16, 64, 192], P(('gx', 'gy')), may hold values from -0.15625 to 0.15625
- block_links: int32 [16, 3], P(('gx', 'gy')), may hold values from 0 to 15, as said below
- top_coupling: bfloat16 [4, 64, 192], P('gx'), may hold values from -0.109375 to 0.109375
- top_links: int32 [4, 3], P('gx'), may hold values from 0 to 3, as said below
Outputs:
- smoothed: float32 [16, 131072], P(None, ('gx', 'gy', 'gz'))
- twice: float32 [16, 131072], P(None, ('gx', 'gy', 'gz'))
The draws below stay inside these ranges and needn't reach their ends.
Inputs may be any that keep to these rules, and one draw needn't show every extreme that they name: `order`: each device's block of 4096 consecutive entries is a permutation of 0 to 4095. `near_list`: row i holds i first, then two different leaves j with 1 <= |j - i| <= 2. `leaf_links`: row i holds three different leaves j with 2 <= |j - i| <= 4. `device_links`: row i holds three different device clusters j with 1 <= |j - i| <= 3. `block_links`: row i holds three different second-level clusters other than i. `top_links`: row i holds three different first-level clusters other than i.
All inputs are finite; a program needn't handle non-finite values.
Results may differ from the reference program's by a relative error of at most 0.0043.
Values may be sent and summed in bfloat16 or wider, within the bound.
No kernel may reach another device: no remote copies, remote signals or barrier semaphores. Data moves between devices by JAX's collectives and lax.ppermute only.
A program may use at most 64 MiB of HBM per device.

```python
import jax
import jax.numpy as jnp
from jax import lax

LEAF = 256
RANK = 64
RHS = 16
LEAF_DEV = 16
NEAR = 3
LINKS = 3
NEAR_REACH = 2
LINK_REACH = 4
DEVICE_REACH = 3
POINT_DEV = 4096
LEAVES = 512
POINTS = 131072
BLOCKS = 16
TOPS = 4
N_GY = 4
N_GZ = 2
DEVICES = 32


def pick_offsets(key, node_count, offsets, chosen):
    row_ids = jnp.arange(node_count, dtype=jnp.int32)[:, None]
    candidates = row_ids + offsets[None, :]
    usable = (candidates >= 0) & (candidates < node_count)
    span_count = offsets.shape[0]
    columns = jnp.arange(span_count, dtype=jnp.int32)[None, :]
    scores = jax.random.randint(key, (node_count, span_count), 0, 4096, dtype=jnp.int32) * span_count + columns
    scores = jnp.where(usable, scores, -1 - columns)
    ranked = jnp.argsort(-scores, axis=1)[:, :chosen]
    return jnp.take_along_axis(candidates, ranked, axis=1).astype(jnp.int32)


def pick_others(key, node_count, chosen):
    columns = jnp.arange(node_count, dtype=jnp.int32)[None, :]
    row_ids = jnp.arange(node_count, dtype=jnp.int32)[:, None]
    scores = jax.random.randint(key, (node_count, node_count), 0, 4096, dtype=jnp.int32) * node_count + columns
    scores = jnp.where(columns == row_ids, -1, scores)
    ranked = jnp.argsort(-scores, axis=1)[:, :chosen]
    return ranked.astype(jnp.int32)


def draw_order(key, part):
    block_count = POINTS // POINT_DEV
    keys_all = jax.random.split(jax.random.fold_in(key, 3), block_count)
    perms = jax.vmap(lambda single: jax.random.permutation(single, POINT_DEV))(keys_all)
    return perms.reshape(POINTS).astype(jnp.int32)


def draw_near_list(key, part):
    offsets = jnp.concatenate([jnp.arange(-NEAR_REACH, 0, dtype=jnp.int32), jnp.arange(1, NEAR_REACH + 1, dtype=jnp.int32)])
    others = pick_offsets(jax.random.fold_in(key, 5), LEAVES, offsets, NEAR - 1)
    itself = jnp.arange(LEAVES, dtype=jnp.int32)[:, None]
    return jnp.concatenate([itself, others], axis=1)


def draw_leaf_links(key, part):
    offsets = jnp.concatenate([jnp.arange(-LINK_REACH, -1, dtype=jnp.int32), jnp.arange(2, LINK_REACH + 1, dtype=jnp.int32)])
    return pick_offsets(jax.random.fold_in(key, 7), LEAVES, offsets, LINKS)


def draw_device_links(key, part):
    offsets = jnp.concatenate([jnp.arange(-DEVICE_REACH, 0, dtype=jnp.int32), jnp.arange(1, DEVICE_REACH + 1, dtype=jnp.int32)])
    return pick_offsets(jax.random.fold_in(key, 9), LEAVES // LEAF_DEV, offsets, LINKS)


def draw_block_links(key, part):
    return pick_others(jax.random.fold_in(key, 11), BLOCKS, LINKS)


def draw_top_links(key, part):
    return pick_others(jax.random.fold_in(key, 13), TOPS, LINKS)


def block_levels(own_key, extent, pieces, smallest, largest):
    gain, own = 1.0, jax.random.fold_in(own_key, 6)
    for position, blocks in pieces:
        steps = jnp.exp(jax.random.uniform(jax.random.fold_in(own, position), (blocks,), jnp.float32, smallest / len(pieces), largest / len(pieces)))
        gain = gain * jnp.repeat(steps, extent[position] // blocks).reshape([-1 if axis == position else 1 for axis in range(len(extent))])
    return gain


def gaussian(key, shape, deviation, bound, shards=(), kind=jnp.bfloat16):
    factor_of = block_levels(key, shape, shards, -0.22, 0.18) if shards else 1.0
    array = jax.random.normal(key, shape, jnp.float32) * deviation * factor_of
    return jnp.minimum(jnp.maximum(array, -bound), bound).astype(kind)


def setup_inputs(seed: int = 0) -> dict:
    key_of = jax.random.split(jax.random.key(seed), 17)
    signal = gaussian(key_of[0], (RHS, POINTS), 1.0, 6.0, ((1, 32),), jnp.float32)
    order = draw_order(jax.random.fold_in(key_of[16], 71), 0)
    near_tiles = gaussian(key_of[2], (LEAVES, NEAR, LEAF, LEAF), (NEAR * LEAF) ** -0.5, 0.21875, ((0, 32),))
    near_list = draw_near_list(jax.random.fold_in(key_of[16], 71), 0)
    leaf_basis = gaussian(key_of[4], (LEAVES, RANK, LEAF), LEAF ** -0.5, 0.375, ((0, 32),))
    leaf_transfer = gaussian(key_of[5], (LEAVES, RANK, RANK), (2 * RANK) ** -0.5, 0.5, ((0, 32),))
    leaf_coupling = gaussian(key_of[6], (LEAVES, RANK, LINKS * RANK), (RANK * LINKS) ** -0.5, 0.4375, ((0, 32),))
    leaf_links = draw_leaf_links(jax.random.fold_in(key_of[16], 71), 0)
    device_transfer = gaussian(key_of[8], (DEVICES, RANK, RANK), (2 * RANK) ** -0.5, 0.5, ((0, 32),))
    device_coupling = gaussian(key_of[9], (DEVICES, RANK, LINKS * RANK), (RANK * LINKS * LEAF_DEV // 2) ** -0.5, 0.15625, ((0, 32),))
    device_links = draw_device_links(jax.random.fold_in(key_of[16], 71), 0)
    block_transfer = gaussian(key_of[11], (BLOCKS, RANK, RANK), (2 * RANK) ** -0.5, 0.5, ((0, 16),))
    block_coupling = gaussian(key_of[12], (BLOCKS, RANK, LINKS * RANK), (RANK * LINKS * LEAF_DEV * N_GZ // 4) ** -0.5, 0.15625, ((0, 16),))
    block_links = draw_block_links(jax.random.fold_in(key_of[16], 71), 0)
    top_coupling = gaussian(key_of[14], (TOPS, RANK, LINKS * RANK), (RANK * LINKS * LEAF_DEV * N_GZ * N_GY // 8) ** -0.5, 0.109375, ((0, 4),))
    top_links = draw_top_links(jax.random.fold_in(key_of[16], 71), 0)
    return {"signal": signal, "order": order, "near_tiles": near_tiles, "near_list": near_list, "leaf_basis": leaf_basis, "leaf_transfer": leaf_transfer, "leaf_coupling": leaf_coupling, "leaf_links": leaf_links, "device_transfer": device_transfer, "device_coupling": device_coupling, "device_links": device_links, "block_transfer": block_transfer, "block_coupling": block_coupling, "block_links": block_links, "top_coupling": top_coupling, "top_links": top_links}


HIGH = lax.Precision.HIGHEST


def couple_all(moments, links, coupling):
    node_count = coupling.shape[0]
    table = coupling.astype(jnp.float32).reshape(node_count, RANK, LINKS, RANK)
    return jnp.einsum('rnjk,nkjm->rnm', moments[:, links], table, precision=HIGH)


def gather_up(child, transfer, group):
    shaped = child.reshape(RHS, -1, group, RANK)
    weights = transfer.astype(jnp.float32).reshape(-1, group, RANK, RANK)
    return jnp.einsum('rngk,ngkm->rnm', shaped, weights, precision=HIGH)


def spread(parent, transfer, group):
    repeated = jnp.repeat(parent, group, axis=1)
    return jnp.einsum('rnm,nkm->rnk', repeated, transfer.astype(jnp.float32), precision=HIGH)


def near_field(leaves, near_tiles, near_list):
    device_count = LEAVES // LEAF_DEV

    def one_block(inputs):
        tiles, lists = inputs
        near_rows = leaves[:, lists].astype(jnp.float32)
        return jnp.einsum('rlns,lnst->rlt', near_rows, tiles.astype(jnp.float32))

    blocks = lax.map(one_block, (near_tiles.reshape(device_count, LEAF_DEV, NEAR, LEAF, LEAF), near_list.reshape(device_count, LEAF_DEV, NEAR)))
    return jnp.transpose(blocks, (1, 0, 2, 3)).reshape(RHS, LEAVES, LEAF)


def apply_matrix(leaves, near_tiles, near_list, leaf_basis, leaf_transfer, leaf_coupling, leaf_links, device_transfer, device_coupling, device_links, block_transfer, block_coupling, block_links, top_coupling, top_links):
    basis_f = leaf_basis.astype(jnp.float32)
    moments = jnp.einsum('rls,lks->rlk', leaves.astype(jnp.float32), basis_f)
    device_moment = gather_up(moments, leaf_transfer, LEAF_DEV)
    block_moment = gather_up(device_moment, device_transfer, N_GZ)
    top_moment = gather_up(block_moment, block_transfer, N_GY)
    top_field = couple_all(top_moment, top_links, top_coupling)
    block_field = couple_all(block_moment, block_links, block_coupling) + spread(top_field, block_transfer, N_GY)
    device_field = couple_all(device_moment, device_links, device_coupling) + spread(block_field, device_transfer, N_GZ)
    leaf_field = couple_all(moments, leaf_links, leaf_coupling) + spread(device_field, leaf_transfer, LEAF_DEV)
    rounded = leaf_field.astype(jnp.bfloat16).astype(jnp.float32)
    far_part = jnp.einsum('rlk,lks->rls', rounded, basis_f)
    return near_field(leaves, near_tiles, near_list) + far_part


def reference(signal, order, near_tiles, near_list, leaf_basis, leaf_transfer, leaf_coupling, leaf_links, device_transfer, device_coupling, device_links, block_transfer, block_coupling, block_links, top_coupling, top_links):
    positions = (jnp.arange(POINTS, dtype=jnp.int32) // POINT_DEV) * POINT_DEV + order.astype(jnp.int32)
    matrices = (near_tiles, near_list, leaf_basis, leaf_transfer, leaf_coupling, leaf_links, device_transfer, device_coupling, device_links, block_transfer, block_coupling, block_links, top_coupling, top_links)
    tree = signal[:, positions].astype(jnp.bfloat16).reshape(RHS, LEAVES, LEAF)
    first = apply_matrix(tree, *matrices)
    second = apply_matrix(first.astype(jnp.bfloat16), *matrices)
    empty = jnp.zeros((RHS, POINTS), jnp.float32)
    smoothed = empty.at[:, positions].set(first.reshape(RHS, POINTS))
    twice = empty.at[:, positions].set(second.reshape(RHS, POINTS))
    return smoothed, twice
```

```python
import functools

import jax
import jax.numpy as jnp
from jax import lax
from jax.experimental import pallas as pl
from jax.experimental.pallas import tpu as pltpu
from jax.sharding import PartitionSpec as P

NEAR_REACH = 2
LINK_REACH = 4
LANES = 128
ROWS = 8
AXES = ("gx", "gy", "gz")
F32 = jnp.float32
BF16 = jnp.bfloat16


def halves(a):
    high = a.astype(BF16)
    low = (a - high.astype(F32)).astype(BF16)
    return jnp.concatenate([high, low], axis=0)


def dot(a, b, transposed=False):
    dims = (((1,), (1 if transposed else 0,)), ((), ()))
    if a.dtype == BF16:
        return lax.dot_general(a, b, dims, preferred_element_type=F32)
    product = lax.dot_general(halves(a), b, dims, preferred_element_type=F32)
    return product[: a.shape[0]] + product[a.shape[0] :]


def dot_nt(a, b):
    return dot(a, b, transposed=True)


def device_index():
    index = jnp.int32(0)
    for axis in AXES:
        index = index * lax.axis_size(axis) + lax.axis_index(axis)
    return index


def permuted(read, index_row, tiles, rhs_count):
    index = jnp.broadcast_to(index_row, (ROWS, LANES))
    lane = index % LANES
    tile = index // LANES
    out = [None] * (rhs_count // ROWS)
    for t in range(tiles):
        here = tile == t
        for b in range(len(out)):
            moved = jnp.take_along_axis(read(b, t), lane, axis=1, mode="promise_in_bounds")
            out[b] = moved if t == 0 else jnp.where(here, moved, out[b])
    return jnp.concatenate(out, axis=0)


def inverse(order_ref, tiles):
    columns = lax.broadcasted_iota(jnp.int32, (LANES, LANES), 0)
    rows = lax.broadcasted_iota(jnp.int32, (tiles, LANES), 0)
    lanes = lax.broadcasted_iota(jnp.int32, (tiles, LANES), 1).astype(F32)
    total = jnp.zeros((2 * tiles, LANES), F32)
    for t in range(tiles):
        row = order_ref[t : t + 1, :]
        at_lane = jnp.where(jnp.broadcast_to(row % LANES, (LANES, LANES)) == columns, 1.0, 0.0)
        at_row = jnp.broadcast_to(row // LANES, (tiles, LANES)) == rows
        place = [jnp.where(at_row, float(t), 0.0), jnp.where(at_row, lanes, 0.0)]
        total += dot_nt(jnp.concatenate(place, axis=0).astype(BF16), at_lane.astype(BF16))
    return (total[:tiles] * LANES + total[tiles:]).astype(jnp.int32)


def upward(values, basis_ref, transfer_ref, device_transfer_ref, block_transfer_ref, outs):
    moment_ref, term_ref, core_ref, chip_ref = outs
    leaf_count = len(values)
    rank = basis_ref.shape[1]
    per_row = LANES // rank
    moments = [dot_nt(values[l], basis_ref[l]) for l in range(leaf_count)]
    for l in range(leaf_count):
        moment_ref[l] = halves(moments[l])
    packed = [
        halves(jnp.concatenate(moments[l : l + per_row], axis=1))
        for l in range(0, leaf_count, per_row)
    ]
    both = dot(jnp.concatenate(packed, axis=1), transfer_ref[...])
    own = both[: both.shape[0] // 2] + both[both.shape[0] // 2 :]
    block = dot(own, device_transfer_ref[0])
    top = dot(block, block_transfer_ref[0])
    half = top.shape[0] // 2
    term = jnp.concatenate(
        [
            jnp.concatenate([own, block], axis=1),
            jnp.concatenate([top[:half], top[half:]], axis=1),
        ],
        axis=0,
    ).astype(BF16)
    term_ref[...] = jnp.broadcast_to(term[None], term_ref.shape)

    def edge(first_value, first_moment):
        pieces = []
        for l in range(first_value, first_value + NEAR_REACH):
            pieces += [values[l][:, c : c + LANES] for c in range(0, values[l].shape[1], LANES)]
        pieces += packed[first_moment // per_row : (first_moment + LINK_REACH) // per_row]
        return jnp.concatenate(pieces, axis=0)

    low = edge(0, 0)
    high = edge(leaf_count - NEAR_REACH, leaf_count - LINK_REACH)
    even = lax.axis_index("gz") % 2 == 0
    core_ref[...] = jnp.where(even, high, low)
    chip_ref[...] = jnp.where(even, low, high)


def start_kernel(*refs):
    signal_buf, sems = refs[-2:]
    kept_count = (len(refs) - 2 - 1 - 5) // 2
    sources = refs[: 1 + kept_count]
    value_ref, *outs = refs[1 + kept_count : 6 + kept_count]
    kept = refs[6 + kept_count : -2]
    order_ref, basis_ref, transfer_ref, device_transfer_ref, block_transfer_ref = kept[:5]
    copies = [
        pltpu.make_async_copy(source, target, sems.at[i])
        for i, (source, target) in enumerate(zip(sources, (signal_buf, *kept), strict=True))
    ]
    for copy in copies:
        copy.start()
    rhs_count, point_count = signal_buf.shape
    tiles = point_count // LANES
    leaf_count, _, leaf = value_ref.shape

    def read(b, t):
        return signal_buf[b * ROWS : (b + 1) * ROWS, t * LANES : (t + 1) * LANES]

    for copy in copies[:2]:
        copy.wait()
    values = []
    for l in range(leaf_count):
        parts = [
            permuted(read, order_ref[t : t + 1, :], tiles, rhs_count)
            for t in range(l * leaf // LANES, (l + 1) * leaf // LANES)
        ]
        value = jnp.concatenate(parts, axis=1).astype(BF16)
        value_ref[l] = value
        values.append(value)
    for copy in copies[2:6]:
        copy.wait()
    upward(values, basis_ref, transfer_ref, device_transfer_ref, block_transfer_ref, outs)
    for copy in copies[6:]:
        copy.wait()


def interior_kernel(second, *refs):
    near_list_ref, leaf_links_ref, value_ref, moment_ref, coupling_ref, tiles_hbm, *refs = refs
    if second:
        leaf_ref, inverse_ref, near_ref, field_ref, edge_tiles, out_hbm, *refs = refs
        tile_buf, sems, out_buf, out_sems = refs
    else:
        order_ref, near_ref, field_ref, edge_tiles, inverse_ref, tile_buf, sems = refs
    leaf_count = value_ref.shape[0]
    rank = moment_ref.shape[2]
    inside = range(NEAR_REACH, leaf_count - NEAR_REACH)
    outside = (*range(NEAR_REACH), *range(leaf_count - NEAR_REACH, leaf_count))
    copies = [
        pltpu.make_async_copy(
            tiles_hbm.at[pl.ds(l, CHUNK)], tile_buf.at[pl.ds(l - NEAR_REACH, CHUNK)], sems.at[i]
        )
        for i, l in enumerate(inside[::CHUNK])
    ]
    for i, l in enumerate((0, leaf_count - NEAR_REACH)):
        source = tiles_hbm.at[pl.ds(l, NEAR_REACH)]
        target = edge_tiles.at[pl.ds(i * NEAR_REACH, NEAR_REACH)]
        copies.append(pltpu.make_async_copy(source, target, sems.at[len(copies)]))
    for copy in copies:
        copy.start()
    first_leaf = device_index() * leaf_count
    linked = range(LINK_REACH, leaf_count - LINK_REACH)
    store_fields(
        field_ref,
        [
            leaf_coupling(moment_ref, leaf_links_ref, coupling_ref, l, -first_leaf)
            for l in linked
        ],
    )
    if second:
        writes = put_back(reader(leaf_ref), inverse_ref, out_hbm, out_buf, out_sems)
    else:
        inverse_ref[...] = inverse(order_ref, order_ref.shape[0])
    for i, l in enumerate(inside):
        if i % CHUNK == 0:
            copies[i // CHUNK].wait()
        near_ref[i] = near_product(value_ref, near_list_ref, tile_buf, l, i, -first_leaf)
    for copy in copies[len(inside) // CHUNK :]:
        copy.wait()
    if second:
        for write in writes:
            write.wait()


def edge_kernel(
    near_list_ref, leaf_links_ref, value_ref, moment_ref, core_ref, chip_ref, coupling_ref,
    tiles_ref, near_ref, field_ref, wide_value, wide_moment
):
    leaf_count, rhs_count, leaf = value_ref.shape
    moment_rows, rank = moment_ref.shape[1:]
    per_row = LANES // rank
    even = lax.axis_index("gz") % 2 == 0
    core, chip = core_ref[...], chip_ref[...]
    above = jnp.where(even, core, chip)
    below = jnp.where(even, chip, core)
    for halo, value_at, moment_at in (
        (below, 0, 0),
        (above, NEAR_REACH + leaf_count, LINK_REACH + leaf_count),
    ):
        row = 0
        for e in range(NEAR_REACH):
            for c in range(0, leaf, LANES):
                wide_value[value_at + e, :, c : c + LANES] = halo[row : row + rhs_count]
                row += rhs_count
        for e in range(LINK_REACH):
            lane = (e % per_row) * rank
            at = row + (e // per_row) * moment_rows
            wide_moment[moment_at + e] = halo[at : at + moment_rows, lane : lane + rank]
    wide_value[NEAR_REACH : NEAR_REACH + leaf_count] = value_ref[...]
    wide_moment[LINK_REACH : LINK_REACH + leaf_count] = moment_ref[...]
    first_leaf = device_index() * leaf_count
    outside = (*range(NEAR_REACH), *range(leaf_count - NEAR_REACH, leaf_count))
    for i, l in enumerate(outside):
        near_ref[i] = near_product(
            wide_value, near_list_ref, tiles_ref, l, i, NEAR_REACH - first_leaf
        )
    outside = (*range(LINK_REACH), *range(leaf_count - LINK_REACH, leaf_count))
    store_fields(
        field_ref,
        [
            leaf_coupling(wide_moment, leaf_links_ref, coupling_ref, l, LINK_REACH - first_leaf)
            for l in outside
        ],
    )


def near_product(value_ref, near_list_ref, tiles_ref, l, slot, shift):
    sources = [value_ref[near_list_ref[k, l] + shift] for k in range(near_list_ref.shape[0])]
    return dot(jnp.concatenate(sources, axis=1), tiles_ref[slot])


def leaf_coupling(moment_ref, leaf_links_ref, coupling_ref, l, shift):
    picked = [moment_ref[leaf_links_ref[k, l] + shift] for k in range(leaf_links_ref.shape[0])]
    return coupled_halves(picked, coupling_ref[l])


def store_fields(field_ref, fields):
    rank = fields[0].shape[1]
    per_row = LANES // rank
    for i in range(0, len(fields), per_row):
        field_ref[:, i * rank : (i + per_row) * rank] = jnp.concatenate(
            fields[i : i + per_row], axis=1
        )


def coupled(picked, coupling):
    rows, rank = picked[0].shape
    product = dot(jnp.concatenate(picked, axis=0), coupling)
    total = sum(
        product[k * rows : (k + 1) * rows, k * rank : (k + 1) * rank] for k in range(len(picked))
    )
    return total


def coupled_halves(picked, coupling):
    both = coupled(picked, coupling)
    return both[: both.shape[0] // 2] + both[both.shape[0] // 2 :]


def applied(
    device_links_ref, block_links_ref, top_links_ref, term_ref, near_ref, field_ref,
    edge_near_ref, edge_field_ref, basis_ref, transfer_ref, device_transfer_ref, device_coupling_ref, block_transfer_ref,
    block_coupling_ref, top_coupling_ref
):
    leaf_count, rank, _ = basis_ref.shape
    rhs_count = near_ref.shape[1]
    gz = lax.axis_size("gz")
    under_top = gz * lax.axis_size("gy")

    def top_moment(t):
        total = sum(
            term_ref[t * under_top + j, rhs_count:, :].astype(F32) for j in range(under_top)
        )
        return jnp.concatenate([total[:, :rank], total[:, rank:]], axis=0)

    def block_moment(c):
        return sum(term_ref[c * gz + j, :rhs_count, rank:].astype(F32) for j in range(gz))

    link_count = device_links_ref.shape[1]
    top_field = coupled([top_moment(top_links_ref[0, k]) for k in range(link_count)], top_coupling_ref[0])
    block_field = coupled(
        [block_moment(block_links_ref[0, k]) for k in range(link_count)], block_coupling_ref[0]
    ) + dot_nt(top_field, block_transfer_ref[0])
    device_field = coupled(
        [term_ref[device_links_ref[0, k], :rhs_count, :rank] for k in range(link_count)],
        device_coupling_ref[0],
    ) + dot_nt(block_field, device_transfer_ref[0])
    edge = LINK_REACH * rank
    leaf_field = jnp.concatenate(
        [edge_field_ref[:, :edge], field_ref[...], edge_field_ref[:, edge:]], axis=1
    )
    field = (leaf_field + dot_nt(device_field, transfer_ref[...])).astype(BF16)
    near = [edge_near_ref[l] for l in range(NEAR_REACH)]
    near += [near_ref[l] for l in range(leaf_count - 2 * NEAR_REACH)]
    near += [edge_near_ref[l] for l in range(NEAR_REACH, 2 * NEAR_REACH)]
    return [
        near[l] + dot(field[:, l * rank : (l + 1) * rank], basis_ref[l])
        for l in range(leaf_count)
    ]


INPUTS = 15


def middle_kernel(*refs):
    ins, (first_ref, value_ref, *outs) = refs[:INPUTS], refs[INPUTS:]
    basis_ref, transfer_ref, device_transfer_ref, _, block_transfer_ref = ins[8:13]
    first = applied(*ins)
    values = []
    for l in range(len(first)):
        first_ref[l] = first[l]
        value = first[l].astype(BF16)
        value_ref[l] = value
        values.append(value)
    upward(values, basis_ref, transfer_ref, device_transfer_ref, block_transfer_ref, outs)


def put_back(read, inverse_ref, out_hbm, out_buf, sems):
    rhs_count, point_count = out_buf.shape
    tiles = point_count // LANES
    part = point_count // sems.shape[0]
    writes = []
    for t in range(tiles):
        out_buf[:, t * LANES : (t + 1) * LANES] = permuted(
            read, inverse_ref[t : t + 1, :], tiles, rhs_count
        )
        if (t + 1) * LANES % part == 0:
            columns = pl.ds((t + 1) * LANES - part, part)
            write = pltpu.make_async_copy(
                out_buf.at[:, columns], out_hbm.at[:, columns], sems.at[len(writes)]
            )
            write.start()
            writes.append(write)
    return writes


def reader(leaf_ref):
    per_leaf = leaf_ref.shape[2] // LANES

    def read(b, t):
        lane = (t % per_leaf) * LANES
        return leaf_ref[t // per_leaf, b * ROWS : (b + 1) * ROWS, lane : lane + LANES]

    return read


def end_kernel(*refs):
    ins, (inverse_ref, out_hbm, second_ref, out_buf, sems) = refs[:INPUTS], refs[INPUTS:]
    second = applied(*ins)
    for l in range(len(second)):
        second_ref[l] = second[l]
    for write in put_back(reader(second_ref), inverse_ref, out_hbm, out_buf, sems):
        write.wait()


VMEM = pl.BlockSpec(memory_space=pltpu.VMEM)
SMEM = pl.BlockSpec(memory_space=pltpu.SMEM)
HBM = pl.BlockSpec(memory_space=pltpu.HBM)
MIB = 1 << 20
CHUNK = 3
PARTS = 4


def call(kernel, name, in_specs, outs, out_specs=None, scratch=(), flops=10**6, limit=24 * MIB):
    return pl.pallas_call(
        kernel,
        name=name,
        in_specs=in_specs,
        out_specs=jax.tree.map(lambda _: VMEM, outs) if out_specs is None else out_specs,
        out_shape=outs,
        scratch_shapes=list(scratch),
        cost_estimate=pl.CostEstimate(flops=flops, bytes_accessed=MIB, transcendentals=0),
        compiler_params=pltpu.CompilerParams(vmem_limit_bytes=limit),
    )


def in_hbm(array):
    return pltpu.with_memory_space_constraint(array, pltpu.HBM)


def exchange(core, chip):
    count = 1
    for axis in AXES:
        count *= lax.axis_size(axis)
    inner = [(i, i ^ 1) for i in range(count)]
    outer = [(i, i + 1 if i % 2 else i - 1) for i in range(1, count - 1)]
    return lax.ppermute(core, AXES, inner), lax.ppermute(chip, AXES, outer)


def shards(
    signal, order, near_tiles, near_list, leaf_basis, leaf_transfer, leaf_coupling, leaf_links,
    device_transfer, device_coupling, device_links, block_transfer, block_coupling, block_links,
    top_coupling, top_links
):
    rhs_count, point_count = signal.shape
    leaf_count, rank, leaf = leaf_basis.shape
    tiles = point_count // LANES
    count = 1
    for axis in AXES:
        count *= lax.axis_size(axis)
    shape = jax.ShapeDtypeStruct
    value_out = shape((leaf_count, rhs_count, leaf), BF16)
    wide_out = shape((leaf_count, rhs_count, leaf), F32)
    points_out = shape((rhs_count, point_count), F32)
    inverse_out = shape((tiles, LANES), jnp.int32)
    halo_rows = NEAR_REACH * rhs_count * leaf // LANES + LINK_REACH * 2 * rhs_count * rank // LANES
    up_outs = (
        shape((leaf_count, 2 * rhs_count, rank), BF16),
        shape((count, rhs_count + rhs_count // 2, LANES), BF16),
        shape((halo_rows, LANES), BF16),
        shape((halo_rows, LANES), BF16),
    )
    kept = (
        order.reshape(tiles, LANES),
        leaf_basis,
        leaf_transfer.reshape(leaf_count * rank, rank),
        device_transfer,
        block_transfer,
        device_coupling,
        block_coupling,
        top_coupling,
        leaf_coupling,
    )
    near_tiles = near_tiles.reshape(leaf_count, -1, leaf)
    lists = (near_list.T, leaf_links.T, device_links, block_links, top_links)
    outs = (value_out,) + up_outs + tuple(shape(k.shape, k.dtype) for k in kept + lists)
    value, moment, term, core, chip, *kept = call(
        start_kernel,
        "start",
        [HBM] * (1 + len(kept + lists)),
        outs,
        out_specs=(VMEM,) * (5 + len(kept)) + (SMEM,) * len(lists),
        scratch=[
            pltpu.VMEM((rhs_count, point_count), F32),
            pltpu.SemaphoreType.DMA((1 + len(kept + lists),)),
        ],
    )(*map(in_hbm, (signal, *kept, *lists)))
    order, basis, transfer, device_transfer, block_transfer, *kept = kept
    device_coupling, block_coupling, top_coupling, coupling, *lists = kept
    near_list, leaf_links, *coarse_links = lists

    inside = leaf_count - 2 * NEAR_REACH
    tile_shape = near_tiles.shape[1:]
    inside_outs = (
        shape((inside, rhs_count, leaf), F32),
        shape((rhs_count, (leaf_count - 2 * LINK_REACH) * rank), F32),
        shape((2 * NEAR_REACH, *tile_shape), BF16),
    )
    edge_outs = (
        shape((2 * NEAR_REACH, rhs_count, leaf), F32),
        shape((rhs_count, 2 * LINK_REACH * rank), F32),
    )
    tile_scratch = [
        pltpu.VMEM((inside, *tile_shape), BF16),
        pltpu.SemaphoreType.DMA((inside // CHUNK + 2,)),
    ]
    out_scratch = [pltpu.VMEM((rhs_count, point_count), F32), pltpu.SemaphoreType.DMA((PARTS,))]
    edge_scratch = [
        pltpu.VMEM((leaf_count + 2 * NEAR_REACH, rhs_count, leaf), BF16),
        pltpu.VMEM((leaf_count + 2 * LINK_REACH, 2 * rhs_count, rank), BF16),
    ]

    def interior(second, last_out, out_spec, scratch, *more):
        return call(
            functools.partial(interior_kernel, second),
            "interior_second" if second else "interior_first",
            [SMEM] * 2 + [VMEM] * 3 + [HBM] + [VMEM] * len(more),
            inside_outs + (last_out,),
            out_specs=(VMEM,) * 3 + (out_spec,),
            scratch=scratch,
            flops=10**8,
        )(near_list, leaf_links, value, moment, coupling, in_hbm(near_tiles), *more)

    def edges(tiles):
        return call(edge_kernel, "edges", [SMEM] * 2 + [VMEM] * 6, edge_outs, scratch=edge_scratch)(
            near_list, leaf_links, value, moment, core, chip, coupling, tiles
        )

    def spread(term):
        return lax.all_to_all(term, AXES, 0, 0)

    coarse = (
        basis, transfer, device_transfer, device_coupling, block_transfer, block_coupling,
        top_coupling,
    )
    core, chip = exchange(core, chip)
    term = spread(term)
    near, field, tiles, inverse_order = interior(False, inverse_out, VMEM, tile_scratch, order)
    edge_near, edge_field = edges(tiles)
    first, value, moment, term, core, chip = call(
        middle_kernel, "middle", [SMEM] * 3 + [VMEM] * 12, (wide_out, value_out) + up_outs
    )(*coarse_links, term, near, field, edge_near, edge_field, *coarse)
    core, chip = exchange(core, chip)
    term = spread(term)
    near, field, tiles, smoothed = interior(
        True, points_out, HBM, tile_scratch + out_scratch, first, inverse_order
    )
    edge_near, edge_field = edges(tiles)
    twice = call(
        end_kernel, "end", [SMEM] * 3 + [VMEM] * 13, points_out, out_specs=HBM,
        scratch=[pltpu.VMEM(wide_out.shape, F32)] + out_scratch,
    )(*coarse_links, term, near, field, edge_near, edge_field, *coarse, inverse_order)
    return smoothed, twice


def solution(mesh):
    every = ("gx", "gy", "gz")
    in_specs = (
        P(None, every),
        P(every),
        P(every, None, None, None),
        P(every, None),
        P(every, None, None),
        P(every, None, None),
        P(every, None, None),
        P(every, None),
        P(every, None, None),
        P(every, None, None),
        P(every, None),
        P(("gx", "gy"), None, None),
        P(("gx", "gy"), None, None),
        P(("gx", "gy"), None),
        P("gx", None, None),
        P("gx", None),
    )
    out_specs = (P(None, every), P(None, every))
    return jax.shard_map(shards, mesh=mesh, in_specs=in_specs, out_specs=out_specs, check_vma=False)
```

```python
import functools

import jax
import jax.numpy as jnp
from jax import lax
from jax.experimental import pallas as pl
from jax.experimental.pallas import tpu as pltpu
from jax.sharding import PartitionSpec as P

NEAR_REACH = 2
LINK_REACH = 4
LANES = 128
ROWS = 8
AXES = ("gx", "gy", "gz")
F32 = jnp.float32
BF16 = jnp.bfloat16


def halves(a):
    high = a.astype(BF16)
    low = (a - high.astype(F32)).astype(BF16)
    return jnp.concatenate([high, low], axis=0)


def dot(a, b, transposed=False):
    dims = (((1,), (1 if transposed else 0,)), ((), ()))
    if a.dtype == BF16:
        return lax.dot_general(a, b, dims, preferred_element_type=F32)
    product = lax.dot_general(halves(a), b, dims, preferred_element_type=F32)
    return product[: a.shape[0]] + product[a.shape[0] :]


def dot_nt(a, b):
    return dot(a, b, transposed=True)


def device_index():
    index = jnp.int32(0)
    for axis in AXES:
        index = index * lax.axis_size(axis) + lax.axis_index(axis)
    return index


def moved_lanes(read, index_row, tiles, rhs_count):
    index = jnp.broadcast_to(index_row, (ROWS, LANES))
    lane = index % LANES
    tile = index // LANES
    out = [None] * (rhs_count // ROWS)
    for t in range(tiles):
        here = tile == t
        for b in range(len(out)):
            moved = jnp.take_along_axis(read(b, t), lane, axis=1, mode="promise_in_bounds")
            out[b] = moved if t == 0 else jnp.where(here, moved, out[b])
    return jnp.concatenate(out, axis=0)


def selected_lanes(table_ref, index_rows, tiles, rhs_count):
    columns = lax.broadcasted_iota(jnp.int32, (LANES, LANES), 0)
    chosen = jnp.concatenate(
        [
            jnp.where(jnp.broadcast_to(row % LANES, (LANES, LANES)) == columns, 1.0, 0.0).astype(BF16)
            for row in index_rows
        ],
        axis=1,
    )
    chosen = jnp.concatenate([chosen] * (table_ref.shape[1] // LANES), axis=0)
    tile = jnp.concatenate(
        [jnp.broadcast_to(row // LANES, (rhs_count, LANES)) for row in index_rows], axis=1
    )
    out = jnp.zeros(tile.shape, F32)
    for first in range(0, tiles, TILE_GROUP):
        rows = table_ref[first * rhs_count : (first + TILE_GROUP) * rhs_count]
        moved = dot(rows, chosen)
        for t in range(TILE_GROUP):
            part = moved[t * rhs_count : (t + 1) * rhs_count]
            out = jnp.where(tile == first + t, part, out)
    return out


def permuted(read, index_ref, table_ref, pattern, rhs_count):
    tiles = index_ref.shape[0]
    for pair in range(tiles // 2):
        rows = [index_ref[t : t + 1, :] for t in (2 * pair, 2 * pair + 1)]
        if pattern[pair % len(pattern)]:
            yield selected_lanes(table_ref, rows, tiles, rhs_count)
        else:
            yield jnp.concatenate(
                [moved_lanes(read, row, tiles, rhs_count) for row in rows], axis=1
            )


def inverse(order_ref, tiles):
    columns = lax.broadcasted_iota(jnp.int32, (LANES, LANES), 0)
    rows = lax.broadcasted_iota(jnp.int32, (tiles, LANES), 0)
    lanes = lax.broadcasted_iota(jnp.int32, (tiles, LANES), 1).astype(F32)
    total = jnp.zeros((2 * tiles, LANES), F32)
    for t in range(tiles):
        row = order_ref[t : t + 1, :]
        at_lane = jnp.where(jnp.broadcast_to(row % LANES, (LANES, LANES)) == columns, 1.0, 0.0)
        at_row = jnp.broadcast_to(row // LANES, (tiles, LANES)) == rows
        place = [jnp.where(at_row, float(t), 0.0), jnp.where(at_row, lanes, 0.0)]
        total += dot_nt(jnp.concatenate(place, axis=0).astype(BF16), at_lane.astype(BF16))
    return (total[:tiles] * LANES + total[tiles:]).astype(jnp.int32)


def upward(values, basis_ref, transfer_ref, device_transfer_ref, block_transfer_ref, outs):
    moment_ref, term_ref, core_ref, chip_ref = outs
    leaf_count = len(values)
    rank = basis_ref.shape[1]
    per_row = LANES // rank
    moments = [dot_nt(values[l], basis_ref[l]) for l in range(leaf_count)]
    packed = [
        halves(jnp.concatenate(moments[l : l + per_row], axis=1))
        for l in range(0, leaf_count, per_row)
    ]
    both = dot(jnp.concatenate(packed, axis=1), transfer_ref[...])
    own = both[: both.shape[0] // 2] + both[both.shape[0] // 2 :]
    block = dot(own, device_transfer_ref[0])
    top = dot(block, block_transfer_ref[0])
    half = top.shape[0] // 2
    term = jnp.concatenate(
        [
            jnp.concatenate([own, block], axis=1),
            jnp.concatenate([top[:half], top[half:]], axis=1),
        ],
        axis=0,
    ).astype(BF16)
    term_ref[...] = jnp.broadcast_to(term[None], term_ref.shape)
    for l in range(leaf_count):
        moment_ref[l] = halves(moments[l])

    def edge(first_value, first_moment):
        pieces = []
        for l in range(first_value, first_value + NEAR_REACH):
            pieces += [values[l][:, c : c + LANES] for c in range(0, values[l].shape[1], LANES)]
        pieces += packed[first_moment // per_row : (first_moment + LINK_REACH) // per_row]
        return jnp.concatenate(pieces, axis=0)

    low = edge(0, 0)
    high = edge(leaf_count - NEAR_REACH, leaf_count - LINK_REACH)
    even = lax.axis_index("gz") % 2 == 0
    core_ref[...] = jnp.where(even, high, low)
    chip_ref[...] = jnp.where(even, low, high)


def start_kernel(*refs):
    signal_buf, sems = refs[-2:]
    kept_count = (len(refs) - 2 - 1 - 5) // 2
    sources = refs[: 1 + kept_count]
    value_ref, *outs = refs[1 + kept_count : 6 + kept_count]
    kept = refs[6 + kept_count : -2]
    order_ref, basis_ref, transfer_ref, device_transfer_ref, block_transfer_ref = kept[:5]
    rhs_count, point_count = signal_buf.shape
    tiles = point_count // LANES
    leaf_count, _, leaf = value_ref.shape
    copies = [
        pltpu.make_async_copy(source, target, sems.at[i])
        for i, (source, target) in enumerate(zip(sources, (signal_buf, *kept), strict=True))
    ]
    for copy in copies:
        copy.start()

    def read(b, t):
        return signal_buf[b * ROWS : (b + 1) * ROWS, t * LANES : (t + 1) * LANES]

    for copy in copies[:2]:
        copy.wait()
    values = []
    for l in range(leaf_count):
        parts = [
            moved_lanes(read, order_ref[t : t + 1, :], tiles, rhs_count)
            for t in range(l * leaf // LANES, (l + 1) * leaf // LANES)
        ]
        value = jnp.concatenate(parts, axis=1).astype(BF16)
        value_ref[l] = value
        values.append(value)
    for copy in copies[2:6]:
        copy.wait()
    upward(
        values, basis_ref, transfer_ref, device_transfer_ref, block_transfer_ref, outs
    )
    for copy in copies[6:]:
        copy.wait()


def interior_kernel(second, *refs):
    near_list_ref, leaf_links_ref, value_ref, moment_ref, coupling_ref, tiles_hbm, *refs = refs
    if second:
        leaf_ref, inverse_ref, near_ref, field_ref, edge_tiles, out_hbm, *refs = refs
        tile_buf, sems, table_ref, out_buf, out_sems = refs
    else:
        order_ref, near_ref, field_ref, edge_tiles, inverse_ref, tile_buf, sems = refs
    leaf_count = value_ref.shape[0]
    inside = range(NEAR_REACH, leaf_count - NEAR_REACH)
    copies = [
        pltpu.make_async_copy(
            tiles_hbm.at[pl.ds(l, CHUNK)], tile_buf.at[pl.ds(l - NEAR_REACH, CHUNK)], sems.at[i]
        )
        for i, l in enumerate(inside[::CHUNK])
    ]
    for i, l in enumerate((0, leaf_count - NEAR_REACH)):
        source = tiles_hbm.at[pl.ds(l, NEAR_REACH)]
        target = edge_tiles.at[pl.ds(i * NEAR_REACH, NEAR_REACH)]
        copies.append(pltpu.make_async_copy(source, target, sems.at[len(copies)]))
    for copy in (*copies[len(inside) // CHUNK :], *copies[: len(inside) // CHUNK]):
        copy.start()
    first_leaf = device_index() * leaf_count
    linked = range(LINK_REACH, leaf_count - LINK_REACH)
    store_fields(
        field_ref,
        [
            leaf_coupling(moment_ref, leaf_links_ref, coupling_ref, l, -first_leaf)
            for l in linked
        ],
    )
    if second:
        values = [leaf_ref[l] for l in range(leaf_count)]
        writes = put_back(values, leaf_ref, inverse_ref, out_hbm, table_ref, out_buf, out_sems)
    else:
        inverse_ref[...] = inverse(order_ref, order_ref.shape[0])
    for i, l in enumerate(inside):
        if i % CHUNK == 0:
            copies[i // CHUNK].wait()
        near_ref[i] = near_product(value_ref, near_list_ref, tile_buf, l, i, -first_leaf)
    for copy in copies[len(inside) // CHUNK :]:
        copy.wait()
    if second:
        for write in writes:
            write.wait()


def edge_kernel(
    near_list_ref, leaf_links_ref, value_ref, moment_ref, core_ref, chip_ref, coupling_ref,
    tiles_ref, near_ref, field_ref, wide_value, wide_moment
):
    leaf_count, rhs_count, leaf = value_ref.shape
    moment_rows, rank = moment_ref.shape[1:]
    per_row = LANES // rank
    even = lax.axis_index("gz") % 2 == 0
    core, chip = core_ref[...], chip_ref[...]
    above = jnp.where(even, core, chip)
    below = jnp.where(even, chip, core)
    for halo, value_at, moment_at in (
        (below, 0, 0),
        (above, NEAR_REACH + leaf_count, LINK_REACH + leaf_count),
    ):
        row = 0
        for e in range(NEAR_REACH):
            for c in range(0, leaf, LANES):
                wide_value[value_at + e, :, c : c + LANES] = halo[row : row + rhs_count]
                row += rhs_count
        for e in range(LINK_REACH):
            lane = (e % per_row) * rank
            at = row + (e // per_row) * moment_rows
            wide_moment[moment_at + e] = halo[at : at + moment_rows, lane : lane + rank]
    wide_value[NEAR_REACH : NEAR_REACH + leaf_count] = value_ref[...]
    wide_moment[LINK_REACH : LINK_REACH + leaf_count] = moment_ref[...]
    first_leaf = device_index() * leaf_count
    outside = (*range(NEAR_REACH), *range(leaf_count - NEAR_REACH, leaf_count))
    for i, l in enumerate(outside):
        near_ref[i] = near_product(
            wide_value, near_list_ref, tiles_ref, l, i, NEAR_REACH - first_leaf
        )
    outside = (*range(LINK_REACH), *range(leaf_count - LINK_REACH, leaf_count))
    store_fields(
        field_ref,
        [
            leaf_coupling(wide_moment, leaf_links_ref, coupling_ref, l, LINK_REACH - first_leaf)
            for l in outside
        ],
    )


def near_product(value_ref, near_list_ref, tiles_ref, l, slot, shift):
    sources = [value_ref[near_list_ref[k, l] + shift] for k in range(near_list_ref.shape[0])]
    return dot(jnp.concatenate(sources, axis=1), tiles_ref[slot])


def leaf_coupling(moment_ref, leaf_links_ref, coupling_ref, l, shift):
    picked = [moment_ref[leaf_links_ref[k, l] + shift] for k in range(leaf_links_ref.shape[0])]
    return coupled_halves(picked, coupling_ref[l])


def store_fields(field_ref, fields):
    rank = fields[0].shape[1]
    per_row = LANES // rank
    for i in range(0, len(fields), per_row):
        field_ref[:, i * rank : (i + per_row) * rank] = jnp.concatenate(
            fields[i : i + per_row], axis=1
        )


def coupled(picked, coupling):
    rows, rank = picked[0].shape
    product = dot(jnp.concatenate(picked, axis=0), coupling)
    total = sum(
        product[k * rows : (k + 1) * rows, k * rank : (k + 1) * rank] for k in range(len(picked))
    )
    return total


def coupled_halves(picked, coupling):
    both = coupled(picked, coupling)
    return both[: both.shape[0] // 2] + both[both.shape[0] // 2 :]


def applied(
    device_links_ref, block_links_ref, top_links_ref, term_ref, near_ref, field_ref,
    edge_near_ref, edge_field_ref, basis_ref, transfer_ref, device_transfer_ref, device_coupling_ref, block_transfer_ref,
    block_coupling_ref, top_coupling_ref
):
    leaf_count, rank, _ = basis_ref.shape
    rhs_count = near_ref.shape[1]
    gz = lax.axis_size("gz")
    under_top = gz * lax.axis_size("gy")

    def top_moment(t):
        total = sum(
            term_ref[t * under_top + j, rhs_count:, :].astype(F32) for j in range(under_top)
        )
        return jnp.concatenate([total[:, :rank], total[:, rank:]], axis=0)

    def block_moment(c):
        return sum(term_ref[c * gz + j, :rhs_count, rank:].astype(F32) for j in range(gz))

    link_count = device_links_ref.shape[1]
    top_field = coupled([top_moment(top_links_ref[0, k]) for k in range(link_count)], top_coupling_ref[0])
    block_field = coupled(
        [block_moment(block_links_ref[0, k]) for k in range(link_count)], block_coupling_ref[0]
    ) + dot_nt(top_field, block_transfer_ref[0])
    device_field = coupled(
        [term_ref[device_links_ref[0, k], :rhs_count, :rank] for k in range(link_count)],
        device_coupling_ref[0],
    ) + dot_nt(block_field, device_transfer_ref[0])
    edge = LINK_REACH * rank
    leaf_field = jnp.concatenate(
        [edge_field_ref[:, :edge], field_ref[...], edge_field_ref[:, edge:]], axis=1
    )
    field = (leaf_field + dot_nt(device_field, transfer_ref[...])).astype(BF16)
    near = [edge_near_ref[l] for l in range(NEAR_REACH)]
    near += [near_ref[l] for l in range(leaf_count - 2 * NEAR_REACH)]
    near += [edge_near_ref[l] for l in range(NEAR_REACH, 2 * NEAR_REACH)]
    return [
        near[l] + dot(field[:, l * rank : (l + 1) * rank], basis_ref[l])
        for l in range(leaf_count)
    ]


INPUTS = 15


def middle_kernel(*refs):
    ins, (first_ref, value_ref, *outs) = refs[:INPUTS], refs[INPUTS:]
    basis_ref, transfer_ref, device_transfer_ref, _, block_transfer_ref = ins[8:13]
    first = applied(*ins)
    values = [leaf_first.astype(BF16) for leaf_first in first]
    upward(values, basis_ref, transfer_ref, device_transfer_ref, block_transfer_ref, outs)
    for l in range(len(first)):
        first_ref[l] = first[l]
        value_ref[l] = values[l]


def put_back(values, leaf_ref, inverse_ref, out_hbm, table_ref, out_buf, sems):
    rhs_count, point_count = out_buf.shape
    per_leaf = leaf_ref.shape[2] // LANES
    part = point_count // sems.shape[0]
    for l in range(len(values)):
        for c in range(per_leaf):
            value = values[l][:, c * LANES : (c + 1) * LANES]
            high = value.astype(BF16)
            low = (value - high.astype(F32)).astype(BF16)
            row = (l * per_leaf + c) * rhs_count
            table_ref[row : row + rhs_count] = jnp.concatenate([high, low], axis=1)

    def read(b, t):
        lane = (t % per_leaf) * LANES
        return leaf_ref[t // per_leaf, b * ROWS : (b + 1) * ROWS, lane : lane + LANES]

    writes = []
    end = 0
    for columns in permuted(read, inverse_ref, table_ref, (True, True, False), rhs_count):
        start, end = end, end + columns.shape[1]
        out_buf[:, start:end] = columns
        if end % part == 0:
            written = pl.ds(end - part, part)
            write = pltpu.make_async_copy(
                out_buf.at[:, written], out_hbm.at[:, written], sems.at[len(writes)]
            )
            write.start()
            writes.append(write)
    return writes


def end_kernel(*refs):
    ins, (inverse_ref, out_hbm, second_ref, *scratch) = refs[:INPUTS], refs[INPUTS:]
    second = applied(*ins)
    for l in range(len(second)):
        second_ref[l] = second[l]
    for write in put_back(second, second_ref, inverse_ref, out_hbm, *scratch):
        write.wait()


VMEM = pl.BlockSpec(memory_space=pltpu.VMEM)
SMEM = pl.BlockSpec(memory_space=pltpu.SMEM)
HBM = pl.BlockSpec(memory_space=pltpu.HBM)
MIB = 1 << 20
CHUNK = 4
PARTS = 4
TILE_GROUP = 8


def call(kernel, name, in_specs, outs, out_specs=None, scratch=(), flops=10**6, limit=24 * MIB):
    return pl.pallas_call(
        kernel,
        name=name,
        in_specs=in_specs,
        out_specs=jax.tree.map(lambda _: VMEM, outs) if out_specs is None else out_specs,
        out_shape=outs,
        scratch_shapes=list(scratch),
        cost_estimate=pl.CostEstimate(flops=flops, bytes_accessed=MIB, transcendentals=0),
        compiler_params=pltpu.CompilerParams(vmem_limit_bytes=limit),
    )


def in_hbm(array):
    return pltpu.with_memory_space_constraint(array, pltpu.HBM)


def exchange(core, chip):
    count = 1
    for axis in AXES:
        count *= lax.axis_size(axis)
    inner = [(i, i ^ 1) for i in range(count)]
    outer = [(i, i + 1 if i % 2 else i - 1) for i in range(1, count - 1)]
    chip = lax.ppermute(chip, AXES, outer)
    return lax.ppermute(core, AXES, inner), chip


def shards(
    signal, order, near_tiles, near_list, leaf_basis, leaf_transfer, leaf_coupling, leaf_links,
    device_transfer, device_coupling, device_links, block_transfer, block_coupling, block_links,
    top_coupling, top_links
):
    rhs_count, point_count = signal.shape
    leaf_count, rank, leaf = leaf_basis.shape
    column_tiles = point_count // LANES
    count = 1
    for axis in AXES:
        count *= lax.axis_size(axis)
    shape = jax.ShapeDtypeStruct
    value_out = shape((leaf_count, rhs_count, leaf), BF16)
    wide_out = shape((leaf_count, rhs_count, leaf), F32)
    points_out = shape((rhs_count, point_count), F32)
    inverse_out = shape((column_tiles, LANES), jnp.int32)
    halo_rows = NEAR_REACH * rhs_count * leaf // LANES + LINK_REACH * 2 * rhs_count * rank // LANES
    up_outs = (
        shape((leaf_count, 2 * rhs_count, rank), BF16),
        shape((count, rhs_count + rhs_count // 2, LANES), BF16),
        shape((halo_rows, LANES), BF16),
        shape((halo_rows, LANES), BF16),
    )
    kept = (
        order.reshape(column_tiles, LANES),
        leaf_basis,
        leaf_transfer.reshape(leaf_count * rank, rank),
        device_transfer,
        block_transfer,
        device_coupling,
        block_coupling,
        top_coupling,
        leaf_coupling,
    )
    near_tiles = near_tiles.reshape(leaf_count, -1, leaf)
    lists = (near_list.T, leaf_links.T, device_links, block_links, top_links)
    tile_shape = near_tiles.shape[1:]
    outs = (value_out,) + up_outs + tuple(shape(k.shape, k.dtype) for k in kept + lists)
    value, moment, term, core, chip, *kept = call(
        start_kernel,
        "start",
        [HBM] * (1 + len(kept + lists)),
        outs,
        out_specs=(VMEM,) * (5 + len(kept)) + (SMEM,) * len(lists),
        scratch=[
            pltpu.VMEM((rhs_count, point_count), F32),
            pltpu.SemaphoreType.DMA((1 + len(kept + lists),)),
        ],
    )(*map(in_hbm, (signal, *kept, *lists)))
    order, basis, transfer, device_transfer, block_transfer, *kept = kept
    device_coupling, block_coupling, top_coupling, coupling, *lists = kept
    near_list, leaf_links, *coarse_links = lists

    inside = leaf_count - 2 * NEAR_REACH
    inside_outs = (
        shape((inside, rhs_count, leaf), F32),
        shape((rhs_count, (leaf_count - 2 * LINK_REACH) * rank), F32),
        shape((2 * NEAR_REACH, *tile_shape), BF16),
    )
    edge_outs = (
        shape((2 * NEAR_REACH, rhs_count, leaf), F32),
        shape((rhs_count, 2 * LINK_REACH * rank), F32),
    )
    tile_scratch = [
        pltpu.VMEM((inside, *tile_shape), BF16),
        pltpu.SemaphoreType.DMA((inside // CHUNK + 2,)),
    ]
    out_scratch = [
        pltpu.VMEM((column_tiles * rhs_count, 2 * LANES), BF16),
        pltpu.VMEM((rhs_count, point_count), F32),
        pltpu.SemaphoreType.DMA((PARTS,)),
    ]
    edge_scratch = [
        pltpu.VMEM((leaf_count + 2 * NEAR_REACH, rhs_count, leaf), BF16),
        pltpu.VMEM((leaf_count + 2 * LINK_REACH, 2 * rhs_count, rank), BF16),
    ]

    def interior(second, last_out, out_spec, scratch, *more):
        return call(
            functools.partial(interior_kernel, second),
            "interior_second" if second else "interior_first",
            [SMEM] * 2 + [VMEM] * 3 + [HBM] + [VMEM] * len(more),
            inside_outs + (last_out,),
            out_specs=(VMEM,) * 3 + (out_spec,),
            scratch=scratch,
            flops=10**8,
        )(near_list, leaf_links, value, moment, coupling, in_hbm(near_tiles), *more)

    def edges(tiles):
        return call(edge_kernel, "edges", [SMEM] * 2 + [VMEM] * 6, edge_outs, scratch=edge_scratch)(
            near_list, leaf_links, value, moment, core, chip, coupling, tiles
        )

    def spread(term):
        return lax.all_to_all(term, AXES, 0, 0)

    coarse = (
        basis, transfer, device_transfer, device_coupling, block_transfer, block_coupling,
        top_coupling,
    )
    core, chip = exchange(core, chip)
    term = spread(term)
    near, field, tiles, inverse_order = interior(False, inverse_out, VMEM, tile_scratch, order)
    edge_near, edge_field = edges(tiles)
    first, value, moment, term, core, chip = call(
        middle_kernel, "middle", [SMEM] * 3 + [VMEM] * 12, (wide_out, value_out) + up_outs,
    )(*coarse_links, term, near, field, edge_near, edge_field, *coarse)
    core, chip = exchange(core, chip)
    term = spread(term)
    near, field, tiles, smoothed = interior(
        True, points_out, HBM, tile_scratch + out_scratch, first, inverse_order
    )
    edge_near, edge_field = edges(tiles)
    twice = call(
        end_kernel, "end", [SMEM] * 3 + [VMEM] * 13, points_out, out_specs=HBM,
        scratch=[pltpu.VMEM(wide_out.shape, F32)] + out_scratch,
    )(*coarse_links, term, near, field, edge_near, edge_field, *coarse, inverse_order)
    return smoothed, twice


def solution(mesh):
    every = ("gx", "gy", "gz")
    in_specs = (
        P(None, every),
        P(every),
        P(every, None, None, None),
        P(every, None),
        P(every, None, None),
        P(every, None, None),
        P(every, None, None),
        P(every, None),
        P(every, None, None),
        P(every, None, None),
        P(every, None),
        P(("gx", "gy"), None, None),
        P(("gx", "gy"), None, None),
        P(("gx", "gy"), None),
        P("gx", None, None),
        P("gx", None),
    )
    out_specs = (P(None, every), P(None, every))
    return jax.shard_map(shards, mesh=mesh, in_specs=in_specs, out_specs=out_specs, check_vma=False)
```

```python
import functools

import jax
import jax.numpy as jnp
from jax import lax
from jax.experimental import pallas as pl
from jax.experimental.pallas import tpu as pltpu
from jax.sharding import PartitionSpec as P

NEAR_REACH = 2
LINK_REACH = 4
LANES = 128
ROWS = 8
AXES = ("gx", "gy", "gz")
F32 = jnp.float32
BF16 = jnp.bfloat16


def halves(a):
    high = a.astype(BF16)
    low = (a - high.astype(F32)).astype(BF16)
    return jnp.concatenate([high, low], axis=0)


def dot(a, b, transposed=False):
    dims = (((1,), (1 if transposed else 0,)), ((), ()))
    if a.dtype == BF16:
        return lax.dot_general(a, b, dims, preferred_element_type=F32)
    product = lax.dot_general(halves(a), b, dims, preferred_element_type=F32)
    return product[: a.shape[0]] + product[a.shape[0] :]


def dot_nt(a, b):
    return dot(a, b, transposed=True)


def device_index():
    index = jnp.int32(0)
    for axis in AXES:
        index = index * lax.axis_size(axis) + lax.axis_index(axis)
    return index


def moved_lanes(read, index_row, tiles, rhs_count):
    index = jnp.broadcast_to(index_row, (ROWS, LANES))
    lane = index % LANES
    tile = index // LANES
    out = [None] * (rhs_count // ROWS)
    for t in range(tiles):
        here = tile == t
        for b in range(len(out)):
            moved = jnp.take_along_axis(read(b, t), lane, axis=1, mode="promise_in_bounds")
            out[b] = moved if t == 0 else jnp.where(here, moved, out[b])
    return jnp.concatenate(out, axis=0)


def selected_lanes(table_ref, index_rows, tiles, rhs_count):
    columns = lax.broadcasted_iota(jnp.int32, (LANES, LANES), 0)
    chosen = jnp.concatenate(
        [
            jnp.where(jnp.broadcast_to(row % LANES, (LANES, LANES)) == columns, 1.0, 0.0).astype(BF16)
            for row in index_rows
        ],
        axis=1,
    )
    chosen = jnp.concatenate([chosen] * (table_ref.shape[1] // LANES), axis=0)
    tile = jnp.concatenate(
        [jnp.broadcast_to(row // LANES, (rhs_count, LANES)) for row in index_rows], axis=1
    )
    out = jnp.zeros(tile.shape, F32)
    for first in range(0, tiles, TILE_GROUP):
        rows = table_ref[first * rhs_count : (first + TILE_GROUP) * rhs_count]
        moved = dot(rows, chosen)
        for t in range(TILE_GROUP):
            part = moved[t * rhs_count : (t + 1) * rhs_count]
            out = jnp.where(tile == first + t, part, out)
    return out


def permuted(read, index_ref, table_ref, pattern, rhs_count):
    tiles = index_ref.shape[0]
    for pair in range(tiles // 2):
        rows = [index_ref[t : t + 1, :] for t in (2 * pair, 2 * pair + 1)]
        if pattern[pair % len(pattern)]:
            yield selected_lanes(table_ref, rows, tiles, rhs_count)
        else:
            yield jnp.concatenate(
                [moved_lanes(read, row, tiles, rhs_count) for row in rows], axis=1
            )


def inverse(order_ref, tiles):
    columns = lax.broadcasted_iota(jnp.int32, (LANES, LANES), 0)
    rows = lax.broadcasted_iota(jnp.int32, (tiles, LANES), 0)
    lanes = lax.broadcasted_iota(jnp.int32, (tiles, LANES), 1).astype(F32)
    total = jnp.zeros((2 * tiles, LANES), F32)
    for t in range(tiles):
        row = order_ref[t : t + 1, :]
        at_lane = jnp.where(jnp.broadcast_to(row % LANES, (LANES, LANES)) == columns, 1.0, 0.0)
        at_row = jnp.broadcast_to(row // LANES, (tiles, LANES)) == rows
        place = [jnp.where(at_row, float(t), 0.0), jnp.where(at_row, lanes, 0.0)]
        total += dot_nt(jnp.concatenate(place, axis=0).astype(BF16), at_lane.astype(BF16))
    return (total[:tiles] * LANES + total[tiles:]).astype(jnp.int32)


def upward(values, basis_ref, transfer_ref, device_transfer_ref, block_transfer_ref, outs):
    moment_ref, term_ref, core_ref, chip_ref = outs
    leaf_count = len(values)
    rank = basis_ref.shape[1]
    per_row = LANES // rank
    moments = [dot_nt(values[l], basis_ref[l]) for l in range(leaf_count)]
    packed = [
        halves(jnp.concatenate(moments[l : l + per_row], axis=1))
        for l in range(0, leaf_count, per_row)
    ]
    both = dot(jnp.concatenate(packed, axis=1), transfer_ref[...])
    own = both[: both.shape[0] // 2] + both[both.shape[0] // 2 :]
    block = dot(own, device_transfer_ref[0])
    top = dot(block, block_transfer_ref[0])
    half = top.shape[0] // 2
    term = jnp.concatenate(
        [
            jnp.concatenate([own, block], axis=1),
            jnp.concatenate([top[:half], top[half:]], axis=1),
        ],
        axis=0,
    ).astype(BF16)
    term_ref[...] = jnp.broadcast_to(term[None], term_ref.shape)
    for l in range(leaf_count):
        moment_ref[l] = halves(moments[l])

    def edge(first_value, first_moment):
        pieces = []
        for l in range(first_value, first_value + NEAR_REACH):
            pieces += [values[l][:, c : c + LANES] for c in range(0, values[l].shape[1], LANES)]
        pieces += packed[first_moment // per_row : (first_moment + LINK_REACH) // per_row]
        return jnp.concatenate(pieces, axis=0)

    low = edge(0, 0)
    high = edge(leaf_count - NEAR_REACH, leaf_count - LINK_REACH)
    even = lax.axis_index("gz") % 2 == 0
    core_ref[...] = jnp.where(even, high, low)
    chip_ref[...] = jnp.where(even, low, high)


def start_kernel(*refs):
    signal_buf, sems = refs[-2:]
    kept_count = (len(refs) - 2 - 1 - 5) // 2
    sources = refs[: 1 + kept_count]
    value_ref, *outs = refs[1 + kept_count : 6 + kept_count]
    kept = refs[6 + kept_count : -2]
    order_ref, basis_ref, transfer_ref, device_transfer_ref, block_transfer_ref = kept[:5]
    rhs_count, point_count = signal_buf.shape
    tiles = point_count // LANES
    leaf_count, _, leaf = value_ref.shape
    copies = [
        pltpu.make_async_copy(source, target, sems.at[i])
        for i, (source, target) in enumerate(zip(sources, (signal_buf, *kept), strict=True))
    ]
    for copy in copies:
        copy.start()

    def read(b, t):
        return signal_buf[b * ROWS : (b + 1) * ROWS, t * LANES : (t + 1) * LANES]

    for copy in copies[:2]:
        copy.wait()
    values = []
    for l in range(leaf_count):
        parts = [
            moved_lanes(read, order_ref[t : t + 1, :], tiles, rhs_count)
            for t in range(l * leaf // LANES, (l + 1) * leaf // LANES)
        ]
        value = jnp.concatenate(parts, axis=1).astype(BF16)
        value_ref[l] = value
        values.append(value)
    for copy in copies[2:6]:
        copy.wait()
    upward(
        values, basis_ref, transfer_ref, device_transfer_ref, block_transfer_ref, outs
    )
    for copy in copies[6:]:
        copy.wait()


def interior_kernel(second, *refs):
    near_list_ref, leaf_links_ref, value_ref, moment_ref, coupling_ref, tiles_hbm, *refs = refs
    if second:
        leaf_ref, inverse_ref, near_ref, field_ref, edge_tiles, out_hbm, *refs = refs
        tile_buf, sems, table_ref, out_buf, out_sems = refs
    else:
        order_ref, near_ref, field_ref, edge_tiles, inverse_ref, tile_buf, sems = refs
    leaf_count = value_ref.shape[0]
    inside = range(NEAR_REACH, leaf_count - NEAR_REACH)
    copies = [
        pltpu.make_async_copy(
            tiles_hbm.at[pl.ds(l, CHUNK)], tile_buf.at[pl.ds(l - NEAR_REACH, CHUNK)], sems.at[i]
        )
        for i, l in enumerate(inside[::CHUNK])
    ]
    for i, l in enumerate((0, leaf_count - NEAR_REACH)):
        source = tiles_hbm.at[pl.ds(l, NEAR_REACH)]
        target = edge_tiles.at[pl.ds(i * NEAR_REACH, NEAR_REACH)]
        copies.append(pltpu.make_async_copy(source, target, sems.at[len(copies)]))
    for copy in (*copies[len(inside) // CHUNK :], *copies[: len(inside) // CHUNK]):
        copy.start()
    first_leaf = device_index() * leaf_count
    linked = range(LINK_REACH, leaf_count - LINK_REACH)
    store_fields(
        field_ref,
        [
            leaf_coupling(moment_ref, leaf_links_ref, coupling_ref, l, -first_leaf)
            for l in linked
        ],
    )
    if second:
        values = [leaf_ref[l] for l in range(leaf_count)]
        writes = put_back(values, leaf_ref, inverse_ref, out_hbm, table_ref, out_buf, out_sems)
    else:
        inverse_ref[...] = inverse(order_ref, order_ref.shape[0])
    for i, l in enumerate(inside):
        if i % CHUNK == 0:
            copies[i // CHUNK].wait()
        near_ref[i] = near_product(value_ref, near_list_ref, tile_buf, l, i, -first_leaf)
    for copy in copies[len(inside) // CHUNK :]:
        copy.wait()
    if second:
        for write in writes:
            write.wait()


def edge_kernel(
    near_list_ref, leaf_links_ref, value_ref, moment_ref, core_ref, chip_ref, coupling_ref,
    tiles_ref, near_ref, field_ref, wide_value, wide_moment
):
    leaf_count, rhs_count, leaf = value_ref.shape
    moment_rows, rank = moment_ref.shape[1:]
    per_row = LANES // rank
    even = lax.axis_index("gz") % 2 == 0
    core, chip = core_ref[...], chip_ref[...]
    above = jnp.where(even, core, chip)
    below = jnp.where(even, chip, core)
    for halo, value_at, moment_at in (
        (below, 0, 0),
        (above, NEAR_REACH + leaf_count, LINK_REACH + leaf_count),
    ):
        row = 0
        for e in range(NEAR_REACH):
            for c in range(0, leaf, LANES):
                wide_value[value_at + e, :, c : c + LANES] = halo[row : row + rhs_count]
                row += rhs_count
        for e in range(LINK_REACH):
            lane = (e % per_row) * rank
            at = row + (e // per_row) * moment_rows
            wide_moment[moment_at + e] = halo[at : at + moment_rows, lane : lane + rank]
    wide_value[NEAR_REACH : NEAR_REACH + leaf_count] = value_ref[...]
    wide_moment[LINK_REACH : LINK_REACH + leaf_count] = moment_ref[...]
    first_leaf = device_index() * leaf_count
    outside = (*range(NEAR_REACH), *range(leaf_count - NEAR_REACH, leaf_count))
    for i, l in enumerate(outside):
        near_ref[i] = near_product(
            wide_value, near_list_ref, tiles_ref, l, i, NEAR_REACH - first_leaf
        )
    outside = (*range(LINK_REACH), *range(leaf_count - LINK_REACH, leaf_count))
    store_fields(
        field_ref,
        [
            leaf_coupling(wide_moment, leaf_links_ref, coupling_ref, l, LINK_REACH - first_leaf)
            for l in outside
        ],
    )


def near_product(value_ref, near_list_ref, tiles_ref, l, slot, shift):
    near_list = near_list_ref[...]
    sources = [value_ref[near_list[k, l] + shift] for k in range(near_list.shape[0])]
    return dot(jnp.concatenate(sources, axis=1), tiles_ref[slot])


def leaf_coupling(moment_ref, leaf_links_ref, coupling_ref, l, shift):
    leaf_links = leaf_links_ref[...]
    picked = [moment_ref[leaf_links[k, l] + shift] for k in range(leaf_links.shape[0])]
    return coupled_halves(picked, coupling_ref[l])


def store_fields(field_ref, fields):
    rank = fields[0].shape[1]
    per_row = LANES // rank
    for i in range(0, len(fields), per_row):
        field_ref[:, i * rank : (i + per_row) * rank] = jnp.concatenate(
            fields[i : i + per_row], axis=1
        )


def coupled(picked, coupling):
    rows, rank = picked[0].shape
    product = dot(jnp.concatenate(picked, axis=0), coupling)
    total = sum(
        product[k * rows : (k + 1) * rows, k * rank : (k + 1) * rank] for k in range(len(picked))
    )
    return total


def coupled_halves(picked, coupling):
    both = coupled(picked, coupling)
    return both[: both.shape[0] // 2] + both[both.shape[0] // 2 :]


def applied(
    device_links_ref, block_links_ref, top_links_ref, term_ref, near_ref, field_ref,
    edge_near_ref, edge_field_ref, basis_ref, transfer_ref, device_transfer_ref, device_coupling_ref, block_transfer_ref,
    block_coupling_ref, top_coupling_ref
):
    leaf_count, rank, _ = basis_ref.shape
    rhs_count = near_ref.shape[1]
    gz = lax.axis_size("gz")
    under_top = gz * lax.axis_size("gy")

    def top_moment(t):
        total = sum(
            term_ref[t * under_top + j, rhs_count:, :].astype(F32) for j in range(under_top)
        )
        return jnp.concatenate([total[:, :rank], total[:, rank:]], axis=0)

    def block_moment(c):
        return sum(term_ref[c * gz + j, :rhs_count, rank:].astype(F32) for j in range(gz))

    device_links, block_links, top_links = (
        device_links_ref[...], block_links_ref[...], top_links_ref[...]
    )
    link_count = device_links.shape[1]
    top_field = coupled([top_moment(top_links[0, k]) for k in range(link_count)], top_coupling_ref[0])
    block_field = coupled(
        [block_moment(block_links[0, k]) for k in range(link_count)], block_coupling_ref[0]
    ) + dot_nt(top_field, block_transfer_ref[0])
    device_field = coupled(
        [term_ref[device_links[0, k], :rhs_count, :rank] for k in range(link_count)],
        device_coupling_ref[0],
    ) + dot_nt(block_field, device_transfer_ref[0])
    edge = LINK_REACH * rank
    leaf_field = jnp.concatenate(
        [edge_field_ref[:, :edge], field_ref[...], edge_field_ref[:, edge:]], axis=1
    )
    field = (leaf_field + dot_nt(device_field, transfer_ref[...])).astype(BF16)
    near = [edge_near_ref[l] for l in range(NEAR_REACH)]
    near += [near_ref[l] for l in range(leaf_count - 2 * NEAR_REACH)]
    near += [edge_near_ref[l] for l in range(NEAR_REACH, 2 * NEAR_REACH)]
    return [
        near[l] + dot(field[:, l * rank : (l + 1) * rank], basis_ref[l])
        for l in range(leaf_count)
    ]


INPUTS = 15


def middle_kernel(*refs):
    ins, (first_ref, value_ref, *outs) = refs[:INPUTS], refs[INPUTS:]
    basis_ref, transfer_ref, device_transfer_ref, _, block_transfer_ref = ins[8:13]
    first = applied(*ins)
    values = [leaf_first.astype(BF16) for leaf_first in first]
    upward(values, basis_ref, transfer_ref, device_transfer_ref, block_transfer_ref, outs)
    for l in range(len(first)):
        first_ref[l] = first[l]
        value_ref[l] = values[l]


def put_back(values, leaf_ref, inverse_ref, out_hbm, table_ref, out_buf, sems):
    rhs_count, point_count = out_buf.shape
    per_leaf = leaf_ref.shape[2] // LANES
    part = point_count // sems.shape[0]
    for l in range(len(values)):
        for c in range(per_leaf):
            value = values[l][:, c * LANES : (c + 1) * LANES]
            high = value.astype(BF16)
            low = (value - high.astype(F32)).astype(BF16)
            row = (l * per_leaf + c) * rhs_count
            table_ref[row : row + rhs_count] = jnp.concatenate([high, low], axis=1)

    def read(b, t):
        lane = (t % per_leaf) * LANES
        return leaf_ref[t // per_leaf, b * ROWS : (b + 1) * ROWS, lane : lane + LANES]

    writes = []
    end = 0
    for columns in permuted(read, inverse_ref, table_ref, (True, True, True, False), rhs_count):
        start, end = end, end + columns.shape[1]
        out_buf[:, start:end] = columns
        if end % part == 0:
            written = pl.ds(end - part, part)
            write = pltpu.make_async_copy(
                out_buf.at[:, written], out_hbm.at[:, written], sems.at[len(writes)]
            )
            write.start()
            writes.append(write)
    return writes


def end_kernel(*refs):
    ins, (inverse_ref, out_hbm, second_ref, *scratch) = refs[:INPUTS], refs[INPUTS:]
    second = applied(*ins)
    for l in range(len(second)):
        second_ref[l] = second[l]
    for write in put_back(second, second_ref, inverse_ref, out_hbm, *scratch):
        write.wait()


VMEM = pl.BlockSpec(memory_space=pltpu.VMEM)
HBM = pl.BlockSpec(memory_space=pltpu.HBM)
MIB = 1 << 20
CHUNK = 4
PARTS = 4
TILE_GROUP = 8


def call(kernel, name, in_specs, outs, out_specs=None, scratch=(), flops=10**6, limit=24 * MIB):
    return pl.pallas_call(
        kernel,
        name=name,
        in_specs=in_specs,
        out_specs=jax.tree.map(lambda _: VMEM, outs) if out_specs is None else out_specs,
        out_shape=outs,
        scratch_shapes=list(scratch),
        cost_estimate=pl.CostEstimate(flops=flops, bytes_accessed=MIB, transcendentals=0),
        compiler_params=pltpu.CompilerParams(vmem_limit_bytes=limit),
    )


def in_hbm(array):
    return pltpu.with_memory_space_constraint(array, pltpu.HBM)


def exchange(core, chip):
    count = 1
    for axis in AXES:
        count *= lax.axis_size(axis)
    inner = [(i, i ^ 1) for i in range(count)]
    outer = [(i, i + 1 if i % 2 else i - 1) for i in range(1, count - 1)]
    chip = lax.ppermute(chip, AXES, outer)
    return lax.ppermute(core, AXES, inner), chip


def shards(
    signal, order, near_tiles, near_list, leaf_basis, leaf_transfer, leaf_coupling, leaf_links,
    device_transfer, device_coupling, device_links, block_transfer, block_coupling, block_links,
    top_coupling, top_links
):
    rhs_count, point_count = signal.shape
    leaf_count, rank, leaf = leaf_basis.shape
    column_tiles = point_count // LANES
    count = 1
    for axis in AXES:
        count *= lax.axis_size(axis)
    shape = jax.ShapeDtypeStruct
    value_out = shape((leaf_count, rhs_count, leaf), BF16)
    wide_out = shape((leaf_count, rhs_count, leaf), F32)
    points_out = shape((rhs_count, point_count), F32)
    inverse_out = shape((column_tiles, LANES), jnp.int32)
    halo_rows = NEAR_REACH * rhs_count * leaf // LANES + LINK_REACH * 2 * rhs_count * rank // LANES
    up_outs = (
        shape((leaf_count, 2 * rhs_count, rank), BF16),
        shape((count, rhs_count + rhs_count // 2, LANES), BF16),
        shape((halo_rows, LANES), BF16),
        shape((halo_rows, LANES), BF16),
    )
    kept = (
        order.reshape(column_tiles, LANES),
        leaf_basis,
        leaf_transfer.reshape(leaf_count * rank, rank),
        device_transfer,
        block_transfer,
        device_coupling,
        block_coupling,
        top_coupling,
        leaf_coupling,
    )
    near_tiles = near_tiles.reshape(leaf_count, -1, leaf)
    lists = (near_list.T, leaf_links.T, device_links, block_links, top_links)
    tile_shape = near_tiles.shape[1:]
    outs = (value_out,) + up_outs + tuple(shape(k.shape, k.dtype) for k in kept + lists)
    value, moment, term, core, chip, *kept = call(
        start_kernel,
        "start",
        [HBM] * (1 + len(kept + lists)),
        outs,
        out_specs=(VMEM,) * (5 + len(kept + lists)),
        scratch=[
            pltpu.VMEM((rhs_count, point_count), F32),
            pltpu.SemaphoreType.DMA((1 + len(kept + lists),)),
        ],
    )(*map(in_hbm, (signal, *kept, *lists)))
    order, basis, transfer, device_transfer, block_transfer, *kept = kept
    device_coupling, block_coupling, top_coupling, coupling, *lists = kept
    near_list, leaf_links, *coarse_links = lists

    inside = leaf_count - 2 * NEAR_REACH
    inside_outs = (
        shape((inside, rhs_count, leaf), F32),
        shape((rhs_count, (leaf_count - 2 * LINK_REACH) * rank), F32),
        shape((2 * NEAR_REACH, *tile_shape), BF16),
    )
    edge_outs = (
        shape((2 * NEAR_REACH, rhs_count, leaf), F32),
        shape((rhs_count, 2 * LINK_REACH * rank), F32),
    )
    tile_scratch = [
        pltpu.VMEM((inside, *tile_shape), BF16),
        pltpu.SemaphoreType.DMA((inside // CHUNK + 2,)),
    ]
    out_scratch = [
        pltpu.VMEM((column_tiles * rhs_count, 2 * LANES), BF16),
        pltpu.VMEM((rhs_count, point_count), F32),
        pltpu.SemaphoreType.DMA((PARTS,)),
    ]
    edge_scratch = [
        pltpu.VMEM((leaf_count + 2 * NEAR_REACH, rhs_count, leaf), BF16),
        pltpu.VMEM((leaf_count + 2 * LINK_REACH, 2 * rhs_count, rank), BF16),
    ]

    def interior(second, last_out, out_spec, scratch, *more):
        return call(
            functools.partial(interior_kernel, second),
            "interior_second" if second else "interior_first",
            [VMEM] * 5 + [HBM] + [VMEM] * len(more),
            inside_outs + (last_out,),
            out_specs=(VMEM,) * 3 + (out_spec,),
            scratch=scratch,
            flops=10**8,
        )(near_list, leaf_links, value, moment, coupling, in_hbm(near_tiles), *more)

    def edges(tiles):
        return call(edge_kernel, "edges", [VMEM] * 8, edge_outs, scratch=edge_scratch)(
            near_list, leaf_links, value, moment, core, chip, coupling, tiles
        )

    def spread(term):
        return lax.all_to_all(term, AXES, 0, 0)

    coarse = (
        basis, transfer, device_transfer, device_coupling, block_transfer, block_coupling,
        top_coupling,
    )
    core, chip = exchange(core, chip)
    term = spread(term)
    near, field, tiles, inverse_order = interior(False, inverse_out, VMEM, tile_scratch, order)
    edge_near, edge_field = edges(tiles)
    first, value, moment, term, core, chip = call(
        middle_kernel, "middle", [VMEM] * 15, (wide_out, value_out) + up_outs,
    )(*coarse_links, term, near, field, edge_near, edge_field, *coarse)
    core, chip = exchange(core, chip)
    term = spread(term)
    near, field, tiles, smoothed = interior(
        True, points_out, HBM, tile_scratch + out_scratch, first, inverse_order
    )
    edge_near, edge_field = edges(tiles)
    twice = call(
        end_kernel, "end", [VMEM] * 16, points_out, out_specs=HBM,
        scratch=[pltpu.VMEM(wide_out.shape, F32)] + out_scratch,
    )(*coarse_links, term, near, field, edge_near, edge_field, *coarse, inverse_order)
    return smoothed, twice


def solution(mesh):
    every = ("gx", "gy", "gz")
    in_specs = (
        P(None, every),
        P(every),
        P(every, None, None, None),
        P(every, None),
        P(every, None, None),
        P(every, None, None),
        P(every, None, None),
        P(every, None),
        P(every, None, None),
        P(every, None, None),
        P(every, None),
        P(("gx", "gy"), None, None),
        P(("gx", "gy"), None, None),
        P(("gx", "gy"), None),
        P("gx", None, None),
        P("gx", None),
    )
    out_specs = (P(None, every), P(None, every))
    return jax.shard_map(shards, mesh=mesh, in_specs=in_specs, out_specs=out_specs, check_vma=False)
```

```python
import functools

import jax
import jax.numpy as jnp
from jax import lax
from jax.experimental import pallas as pl
from jax.experimental.pallas import tpu as pltpu
from jax.sharding import PartitionSpec as P

NEAR_REACH = 2
LINK_REACH = 4
LANES = 128
ROWS = 8
AXES = ("gx", "gy", "gz")
F32 = jnp.float32
BF16 = jnp.bfloat16


def halves(a):
    high = a.astype(BF16)
    low = (a - high.astype(F32)).astype(BF16)
    return jnp.concatenate([high, low], axis=0)


def dot(a, b, transposed=False):
    dims = (((1,), (1 if transposed else 0,)), ((), ()))
    if a.dtype == BF16:
        return lax.dot_general(a, b, dims, preferred_element_type=F32)
    product = lax.dot_general(halves(a), b, dims, preferred_element_type=F32)
    return product[: a.shape[0]] + product[a.shape[0] :]


def dot_nt(a, b):
    return dot(a, b, transposed=True)


def device_index():
    index = jnp.int32(0)
    for axis in AXES:
        index = index * lax.axis_size(axis) + lax.axis_index(axis)
    return index


def moved_lanes(read, index_row, tiles, rhs_count):
    index = jnp.broadcast_to(index_row, (ROWS, LANES))
    lane = index % LANES
    tile = index // LANES
    out = [None] * (rhs_count // ROWS)
    for t in range(tiles):
        here = tile == t
        for b in range(len(out)):
            moved = jnp.take_along_axis(read(b, t), lane, axis=1, mode="promise_in_bounds")
            out[b] = moved if t == 0 else jnp.where(here, moved, out[b])
    return jnp.concatenate(out, axis=0)


def selected_lanes(table_ref, index_rows, tiles, rhs_count):
    columns = lax.broadcasted_iota(jnp.int32, (LANES, LANES), 0)
    chosen = jnp.concatenate(
        [
            jnp.where(jnp.broadcast_to(row % LANES, (LANES, LANES)) == columns, 1.0, 0.0).astype(BF16)
            for row in index_rows
        ],
        axis=1,
    )
    chosen = jnp.concatenate([chosen] * (table_ref.shape[1] // LANES), axis=0)
    tile = jnp.concatenate(
        [jnp.broadcast_to(row // LANES, (rhs_count, LANES)) for row in index_rows], axis=1
    )
    out = jnp.zeros(tile.shape, F32)
    for first in range(0, tiles, TILE_GROUP):
        rows = table_ref[first * rhs_count : (first + TILE_GROUP) * rhs_count]
        moved = dot(rows, chosen)
        for t in range(TILE_GROUP):
            part = moved[t * rhs_count : (t + 1) * rhs_count]
            out = jnp.where(tile == first + t, part, out)
    return out


def permuted(read, index_ref, table_ref, pattern, rhs_count):
    tiles = index_ref.shape[0]
    for pair in range(tiles // 2):
        rows = [index_ref[t : t + 1, :] for t in (2 * pair, 2 * pair + 1)]
        if pattern[pair % len(pattern)]:
            yield selected_lanes(table_ref, rows, tiles, rhs_count)
        else:
            yield jnp.concatenate(
                [moved_lanes(read, row, tiles, rhs_count) for row in rows], axis=1
            )


def inverse(order_ref, tiles):
    columns = lax.broadcasted_iota(jnp.int32, (LANES, LANES), 0)
    rows = lax.broadcasted_iota(jnp.int32, (tiles, LANES), 0)
    lanes = lax.broadcasted_iota(jnp.int32, (tiles, LANES), 1).astype(F32)
    total = jnp.zeros((2 * tiles, LANES), F32)
    for t in range(tiles):
        row = order_ref[t : t + 1, :]
        at_lane = jnp.where(jnp.broadcast_to(row % LANES, (LANES, LANES)) == columns, 1.0, 0.0)
        at_row = jnp.broadcast_to(row // LANES, (tiles, LANES)) == rows
        place = [jnp.where(at_row, float(t), 0.0), jnp.where(at_row, lanes, 0.0)]
        total += dot_nt(jnp.concatenate(place, axis=0).astype(BF16), at_lane.astype(BF16))
    return (total[:tiles] * LANES + total[tiles:]).astype(jnp.int32)


def upward(values, basis_ref, transfer_ref, device_transfer_ref, block_transfer_ref, outs):
    moment_ref, term_ref, core_ref, chip_ref = outs
    leaf_count = len(values)
    rank = basis_ref.shape[1]
    per_row = LANES // rank
    moments = [dot_nt(values[l], basis_ref[l]) for l in range(leaf_count)]
    packed = [
        halves(jnp.concatenate(moments[l : l + per_row], axis=1))
        for l in range(0, leaf_count, per_row)
    ]
    both = dot(jnp.concatenate(packed, axis=1), transfer_ref[...])
    own = both[: both.shape[0] // 2] + both[both.shape[0] // 2 :]
    block = dot(own, device_transfer_ref[0])
    top = dot(block, block_transfer_ref[0])
    half = top.shape[0] // 2
    term = jnp.concatenate(
        [
            jnp.concatenate([own, block], axis=1),
            jnp.concatenate([top[:half], top[half:]], axis=1),
        ],
        axis=0,
    ).astype(BF16)
    term_ref[...] = jnp.broadcast_to(term[None], term_ref.shape)
    for l in range(leaf_count):
        moment_ref[l] = halves(moments[l])

    def edge(first_value, first_moment):
        pieces = []
        for l in range(first_value, first_value + NEAR_REACH):
            pieces += [values[l][:, c : c + LANES] for c in range(0, values[l].shape[1], LANES)]
        pieces += packed[first_moment // per_row : (first_moment + LINK_REACH) // per_row]
        return jnp.concatenate(pieces, axis=0)

    low = edge(0, 0)
    high = edge(leaf_count - NEAR_REACH, leaf_count - LINK_REACH)
    even = lax.axis_index("gz") % 2 == 0
    core_ref[...] = jnp.where(even, high, low)
    chip_ref[...] = jnp.where(even, low, high)


def start_kernel(*refs):
    signal_buf, table_ref, sems = refs[-3:]
    kept_count = (len(refs) - 3 - 1 - 5) // 2
    sources = refs[: 1 + kept_count]
    value_ref, *outs = refs[1 + kept_count : 6 + kept_count]
    kept = refs[6 + kept_count : -3]
    order_ref, basis_ref, transfer_ref, device_transfer_ref, block_transfer_ref = kept[:5]
    rhs_count, point_count = signal_buf.shape
    tiles = point_count // LANES
    leaf_count, _, leaf = value_ref.shape
    copies = [
        pltpu.make_async_copy(source, target, sems.at[i])
        for i, (source, target) in enumerate(zip(sources, (signal_buf, *kept), strict=True))
    ]
    for copy in copies:
        copy.start()

    def read(b, t):
        return signal_buf[b * ROWS : (b + 1) * ROWS, t * LANES : (t + 1) * LANES]

    for copy in copies[:2]:
        copy.wait()
    for t in range(tiles):
        columns = signal_buf[:, t * LANES : (t + 1) * LANES]
        table_ref[t * rhs_count : (t + 1) * rhs_count] = columns.astype(BF16)
    parts = list(permuted(read, order_ref, table_ref, (True, False), rhs_count))
    per_leaf = len(parts) // leaf_count
    values = []
    for l in range(leaf_count):
        value = jnp.concatenate(parts[l * per_leaf : (l + 1) * per_leaf], axis=1).astype(BF16)
        value_ref[l] = value
        values.append(value)
    for copy in copies[2:6]:
        copy.wait()
    upward(
        values, basis_ref, transfer_ref, device_transfer_ref, block_transfer_ref, outs
    )
    for copy in copies[6:]:
        copy.wait()


def interior_kernel(second, *refs):
    near_list_ref, leaf_links_ref, value_ref, moment_ref, coupling_ref, tiles_hbm, *refs = refs
    if second:
        leaf_ref, inverse_ref, near_ref, field_ref, edge_tiles, out_hbm, *refs = refs
        tile_buf, sems, table_ref, out_buf, out_sems = refs
    else:
        order_ref, near_ref, field_ref, edge_tiles, inverse_ref, tile_buf, sems = refs
    leaf_count = value_ref.shape[0]
    inside = range(NEAR_REACH, leaf_count - NEAR_REACH)
    copies = [
        pltpu.make_async_copy(
            tiles_hbm.at[pl.ds(l, CHUNK)], tile_buf.at[pl.ds(l - NEAR_REACH, CHUNK)], sems.at[i]
        )
        for i, l in enumerate(inside[::CHUNK])
    ]
    for i, l in enumerate((0, leaf_count - NEAR_REACH)):
        source = tiles_hbm.at[pl.ds(l, NEAR_REACH)]
        target = edge_tiles.at[pl.ds(i * NEAR_REACH, NEAR_REACH)]
        copies.append(pltpu.make_async_copy(source, target, sems.at[len(copies)]))
    for copy in (*copies[len(inside) // CHUNK :], *copies[: len(inside) // CHUNK]):
        copy.start()
    first_leaf = device_index() * leaf_count
    linked = range(LINK_REACH, leaf_count - LINK_REACH)
    store_fields(
        field_ref,
        [
            leaf_coupling(moment_ref, leaf_links_ref, coupling_ref, l, -first_leaf)
            for l in linked
        ],
    )
    if second:
        values = [leaf_ref[l] for l in range(leaf_count)]
        writes = put_back(values, leaf_ref, inverse_ref, out_hbm, table_ref, out_buf, out_sems)
    else:
        inverse_ref[...] = inverse(order_ref, order_ref.shape[0])
    for i, l in enumerate(inside):
        if i % CHUNK == 0:
            copies[i // CHUNK].wait()
        near_ref[i] = near_product(value_ref, near_list_ref, tile_buf, l, i, -first_leaf)
    for copy in copies[len(inside) // CHUNK :]:
        copy.wait()
    if second:
        for write in writes:
            write.wait()


def edge_kernel(
    near_list_ref, leaf_links_ref, value_ref, moment_ref, core_ref, chip_ref, coupling_ref,
    tiles_ref, near_ref, field_ref, wide_value, wide_moment
):
    leaf_count, rhs_count, leaf = value_ref.shape
    moment_rows, rank = moment_ref.shape[1:]
    per_row = LANES // rank
    even = lax.axis_index("gz") % 2 == 0
    core, chip = core_ref[...], chip_ref[...]
    above = jnp.where(even, core, chip)
    below = jnp.where(even, chip, core)
    for halo, value_at, moment_at in (
        (below, 0, 0),
        (above, NEAR_REACH + leaf_count, LINK_REACH + leaf_count),
    ):
        row = 0
        for e in range(NEAR_REACH):
            for c in range(0, leaf, LANES):
                wide_value[value_at + e, :, c : c + LANES] = halo[row : row + rhs_count]
                row += rhs_count
        for e in range(LINK_REACH):
            lane = (e % per_row) * rank
            at = row + (e // per_row) * moment_rows
            wide_moment[moment_at + e] = halo[at : at + moment_rows, lane : lane + rank]
    wide_value[NEAR_REACH : NEAR_REACH + leaf_count] = value_ref[...]
    wide_moment[LINK_REACH : LINK_REACH + leaf_count] = moment_ref[...]
    first_leaf = device_index() * leaf_count
    outside = (*range(NEAR_REACH), *range(leaf_count - NEAR_REACH, leaf_count))
    for i, l in enumerate(outside):
        near_ref[i] = near_product(
            wide_value, near_list_ref, tiles_ref, l, i, NEAR_REACH - first_leaf
        )
    outside = (*range(LINK_REACH), *range(leaf_count - LINK_REACH, leaf_count))
    store_fields(
        field_ref,
        [
            leaf_coupling(wide_moment, leaf_links_ref, coupling_ref, l, LINK_REACH - first_leaf)
            for l in outside
        ],
    )


def near_product(value_ref, near_list_ref, tiles_ref, l, slot, shift):
    near_list = near_list_ref[...]
    sources = [value_ref[near_list[k, l] + shift] for k in range(near_list.shape[0])]
    return dot(jnp.concatenate(sources, axis=1), tiles_ref[slot])


def leaf_coupling(moment_ref, leaf_links_ref, coupling_ref, l, shift):
    leaf_links = leaf_links_ref[...]
    picked = [moment_ref[leaf_links[k, l] + shift] for k in range(leaf_links.shape[0])]
    return coupled_halves(picked, coupling_ref[l])


def store_fields(field_ref, fields):
    rank = fields[0].shape[1]
    per_row = LANES // rank
    for i in range(0, len(fields), per_row):
        field_ref[:, i * rank : (i + per_row) * rank] = jnp.concatenate(
            fields[i : i + per_row], axis=1
        )


def coupled(picked, coupling):
    rows, rank = picked[0].shape
    product = dot(jnp.concatenate(picked, axis=0), coupling)
    total = sum(
        product[k * rows : (k + 1) * rows, k * rank : (k + 1) * rank] for k in range(len(picked))
    )
    return total


def coupled_halves(picked, coupling):
    both = coupled(picked, coupling)
    return both[: both.shape[0] // 2] + both[both.shape[0] // 2 :]


def applied(
    device_links_ref, block_links_ref, top_links_ref, term_ref, near_ref, field_ref,
    edge_near_ref, edge_field_ref, basis_ref, transfer_ref, device_transfer_ref, device_coupling_ref, block_transfer_ref,
    block_coupling_ref, top_coupling_ref
):
    leaf_count, rank, _ = basis_ref.shape
    rhs_count = near_ref.shape[1]
    gz = lax.axis_size("gz")
    under_top = gz * lax.axis_size("gy")

    def top_moment(t):
        total = sum(
            term_ref[t * under_top + j, rhs_count:, :].astype(F32) for j in range(under_top)
        )
        return jnp.concatenate([total[:, :rank], total[:, rank:]], axis=0)

    def block_moment(c):
        return sum(term_ref[c * gz + j, :rhs_count, rank:].astype(F32) for j in range(gz))

    device_links, block_links, top_links = (
        device_links_ref[...], block_links_ref[...], top_links_ref[...]
    )
    link_count = device_links.shape[1]
    top_field = coupled([top_moment(top_links[0, k]) for k in range(link_count)], top_coupling_ref[0])
    block_field = coupled(
        [block_moment(block_links[0, k]) for k in range(link_count)], block_coupling_ref[0]
    ) + dot_nt(top_field, block_transfer_ref[0])
    device_field = coupled(
        [term_ref[device_links[0, k], :rhs_count, :rank] for k in range(link_count)],
        device_coupling_ref[0],
    ) + dot_nt(block_field, device_transfer_ref[0])
    edge = LINK_REACH * rank
    leaf_field = jnp.concatenate(
        [edge_field_ref[:, :edge], field_ref[...], edge_field_ref[:, edge:]], axis=1
    )
    field = (leaf_field + dot_nt(device_field, transfer_ref[...])).astype(BF16)
    near = [edge_near_ref[l] for l in range(NEAR_REACH)]
    near += [near_ref[l] for l in range(leaf_count - 2 * NEAR_REACH)]
    near += [edge_near_ref[l] for l in range(NEAR_REACH, 2 * NEAR_REACH)]
    return [
        near[l] + dot(field[:, l * rank : (l + 1) * rank], basis_ref[l])
        for l in range(leaf_count)
    ]


INPUTS = 15


def middle_kernel(*refs):
    ins, (first_ref, value_ref, *outs) = refs[:INPUTS], refs[INPUTS:]
    basis_ref, transfer_ref, device_transfer_ref, _, block_transfer_ref = ins[8:13]
    first = applied(*ins)
    values = [leaf_first.astype(BF16) for leaf_first in first]
    upward(values, basis_ref, transfer_ref, device_transfer_ref, block_transfer_ref, outs)
    for l in range(len(first)):
        first_ref[l] = first[l]
        value_ref[l] = values[l]


def put_back(values, leaf_ref, inverse_ref, out_hbm, table_ref, out_buf, sems):
    rhs_count, point_count = out_buf.shape
    per_leaf = leaf_ref.shape[2] // LANES
    part = point_count // sems.shape[0]
    for l in range(len(values)):
        for c in range(per_leaf):
            value = values[l][:, c * LANES : (c + 1) * LANES]
            high = value.astype(BF16)
            low = (value - high.astype(F32)).astype(BF16)
            row = (l * per_leaf + c) * rhs_count
            table_ref[row : row + rhs_count] = jnp.concatenate([high, low], axis=1)

    def read(b, t):
        lane = (t % per_leaf) * LANES
        return leaf_ref[t // per_leaf, b * ROWS : (b + 1) * ROWS, lane : lane + LANES]

    writes = []
    end = 0
    for columns in permuted(read, inverse_ref, table_ref, (True, True, True, False), rhs_count):
        start, end = end, end + columns.shape[1]
        out_buf[:, start:end] = columns
        if end % part == 0:
            written = pl.ds(end - part, part)
            write = pltpu.make_async_copy(
                out_buf.at[:, written], out_hbm.at[:, written], sems.at[len(writes)]
            )
            write.start()
            writes.append(write)
    return writes


def end_kernel(*refs):
    ins, (inverse_ref, out_hbm, second_ref, *scratch) = refs[:INPUTS], refs[INPUTS:]
    second = applied(*ins)
    for l in range(len(second)):
        second_ref[l] = second[l]
    for write in put_back(second, second_ref, inverse_ref, out_hbm, *scratch):
        write.wait()


VMEM = pl.BlockSpec(memory_space=pltpu.VMEM)
HBM = pl.BlockSpec(memory_space=pltpu.HBM)
MIB = 1 << 20
CHUNK = 4
PARTS = 4
TILE_GROUP = 8


def call(kernel, name, in_specs, outs, out_specs=None, scratch=(), flops=10**6, limit=24 * MIB):
    return pl.pallas_call(
        kernel,
        name=name,
        in_specs=in_specs,
        out_specs=jax.tree.map(lambda _: VMEM, outs) if out_specs is None else out_specs,
        out_shape=outs,
        scratch_shapes=list(scratch),
        cost_estimate=pl.CostEstimate(flops=flops, bytes_accessed=MIB, transcendentals=0),
        compiler_params=pltpu.CompilerParams(vmem_limit_bytes=limit),
    )


def in_hbm(array):
    return pltpu.with_memory_space_constraint(array, pltpu.HBM)


def exchange(core, chip):
    count = 1
    for axis in AXES:
        count *= lax.axis_size(axis)
    inner = [(i, i ^ 1) for i in range(count)]
    outer = [(i, i + 1 if i % 2 else i - 1) for i in range(1, count - 1)]
    chip = lax.ppermute(chip, AXES, outer)
    return lax.ppermute(core, AXES, inner), chip


def shards(
    signal, order, near_tiles, near_list, leaf_basis, leaf_transfer, leaf_coupling, leaf_links,
    device_transfer, device_coupling, device_links, block_transfer, block_coupling, block_links,
    top_coupling, top_links
):
    rhs_count, point_count = signal.shape
    leaf_count, rank, leaf = leaf_basis.shape
    column_tiles = point_count // LANES
    count = 1
    for axis in AXES:
        count *= lax.axis_size(axis)
    shape = jax.ShapeDtypeStruct
    value_out = shape((leaf_count, rhs_count, leaf), BF16)
    wide_out = shape((leaf_count, rhs_count, leaf), F32)
    points_out = shape((rhs_count, point_count), F32)
    inverse_out = shape((column_tiles, LANES), jnp.int32)
    halo_rows = NEAR_REACH * rhs_count * leaf // LANES + LINK_REACH * 2 * rhs_count * rank // LANES
    up_outs = (
        shape((leaf_count, 2 * rhs_count, rank), BF16),
        shape((count, rhs_count + rhs_count // 2, LANES), BF16),
        shape((halo_rows, LANES), BF16),
        shape((halo_rows, LANES), BF16),
    )
    kept = (
        order.reshape(column_tiles, LANES),
        leaf_basis,
        leaf_transfer.reshape(leaf_count * rank, rank),
        device_transfer,
        block_transfer,
        device_coupling,
        block_coupling,
        top_coupling,
        leaf_coupling,
    )
    near_tiles = near_tiles.reshape(leaf_count, -1, leaf)
    lists = (near_list.T, leaf_links.T, device_links, block_links, top_links)
    tile_shape = near_tiles.shape[1:]
    outs = (value_out,) + up_outs + tuple(shape(k.shape, k.dtype) for k in kept + lists)
    value, moment, term, core, chip, *kept = call(
        start_kernel,
        "start",
        [HBM] * (1 + len(kept + lists)),
        outs,
        out_specs=(VMEM,) * (5 + len(kept + lists)),
        scratch=[
            pltpu.VMEM((rhs_count, point_count), F32),
            pltpu.VMEM((column_tiles * rhs_count, LANES), BF16),
            pltpu.SemaphoreType.DMA((1 + len(kept + lists),)),
        ],
    )(*map(in_hbm, (signal, *kept, *lists)))
    order, basis, transfer, device_transfer, block_transfer, *kept = kept
    device_coupling, block_coupling, top_coupling, coupling, *lists = kept
    near_list, leaf_links, *coarse_links = lists

    inside = leaf_count - 2 * NEAR_REACH
    inside_outs = (
        shape((inside, rhs_count, leaf), F32),
        shape((rhs_count, (leaf_count - 2 * LINK_REACH) * rank), F32),
        shape((2 * NEAR_REACH, *tile_shape), BF16),
    )
    edge_outs = (
        shape((2 * NEAR_REACH, rhs_count, leaf), F32),
        shape((rhs_count, 2 * LINK_REACH * rank), F32),
    )
    tile_scratch = [
        pltpu.VMEM((inside, *tile_shape), BF16),
        pltpu.SemaphoreType.DMA((inside // CHUNK + 2,)),
    ]
    out_scratch = [
        pltpu.VMEM((column_tiles * rhs_count, 2 * LANES), BF16),
        pltpu.VMEM((rhs_count, point_count), F32),
        pltpu.SemaphoreType.DMA((PARTS,)),
    ]
    edge_scratch = [
        pltpu.VMEM((leaf_count + 2 * NEAR_REACH, rhs_count, leaf), BF16),
        pltpu.VMEM((leaf_count + 2 * LINK_REACH, 2 * rhs_count, rank), BF16),
    ]

    def interior(second, last_out, out_spec, scratch, *more):
        return call(
            functools.partial(interior_kernel, second),
            "interior_second" if second else "interior_first",
            [VMEM] * 5 + [HBM] + [VMEM] * len(more),
            inside_outs + (last_out,),
            out_specs=(VMEM,) * 3 + (out_spec,),
            scratch=scratch,
            flops=10**8,
        )(near_list, leaf_links, value, moment, coupling, in_hbm(near_tiles), *more)

    def edges(tiles):
        return call(edge_kernel, "edges", [VMEM] * 8, edge_outs, scratch=edge_scratch)(
            near_list, leaf_links, value, moment, core, chip, coupling, tiles
        )

    def spread(term):
        return lax.all_to_all(term, AXES, 0, 0)

    coarse = (
        basis, transfer, device_transfer, device_coupling, block_transfer, block_coupling,
        top_coupling,
    )
    core, chip = exchange(core, chip)
    term = spread(term)
    near, field, tiles, inverse_order = interior(False, inverse_out, VMEM, tile_scratch, order)
    edge_near, edge_field = edges(tiles)
    first, value, moment, term, core, chip = call(
        middle_kernel, "middle", [VMEM] * 15, (wide_out, value_out) + up_outs,
    )(*coarse_links, term, near, field, edge_near, edge_field, *coarse)
    core, chip = exchange(core, chip)
    term = spread(term)
    near, field, tiles, smoothed = interior(
        True, points_out, HBM, tile_scratch + out_scratch, first, inverse_order
    )
    edge_near, edge_field = edges(tiles)
    twice = call(
        end_kernel, "end", [VMEM] * 16, points_out, out_specs=HBM,
        scratch=[pltpu.VMEM(wide_out.shape, F32)] + out_scratch,
    )(*coarse_links, term, near, field, edge_near, edge_field, *coarse, inverse_order)
    return smoothed, twice


def solution(mesh):
    every = ("gx", "gy", "gz")
    in_specs = (
        P(None, every),
        P(every),
        P(every, None, None, None),
        P(every, None),
        P(every, None, None),
        P(every, None, None),
        P(every, None, None),
        P(every, None),
        P(every, None, None),
        P(every, None, None),
        P(every, None),
        P(("gx", "gy"), None, None),
        P(("gx", "gy"), None, None),
        P(("gx", "gy"), None),
        P("gx", None, None),
        P("gx", None),
    )
    out_specs = (P(None, every), P(None, every))
    return jax.shard_map(shards, mesh=mesh, in_specs=in_specs, out_specs=out_specs, check_vma=False)
```
